128 devices in a mesh: dp: 64 (over z_hi, x, y, core), mp: 2 (over z_lo).
Axes of the slice: x: 4, y: 4, z: 4 (z_hi: 2, z_lo: 2; z = z_hi * 2 + z_lo), core: 2. Of those that a mesh axis runs over, the one named last changes fastest.
Arguments:
- clean: float32 [256, 3, 4096], P(('dp', 'mp')), may hold values from -1 to 1
- noise: float32 [256, 3, 4096], P(('dp', 'mp')), may hold values from -12 to 12
- lowres: float32 [256, 3, 4096], P(('dp', 'mp')), may hold values from -1 to 1
- aug_noise: float32 [256, 3, 4096], P(('dp', 'mp')), may hold values from -5 to 5
- timesteps: int32 [256], P(('dp', 'mp')), may hold values from 0 to 999
- aug_levels: int32 [256], P(('dp', 'mp')), may hold values from 0 to 999
- lengths: int32 [256], P(('dp', 'mp')), may hold values from 1 to 128
- text: bfloat16 [256, 128, 4096], P(('dp', 'mp')), may hold values from -160 to 160
- w_stem: float32 [6, 128], replicated, may hold values from -2.5 to 2.5
- w_time: float32 [256, 256], replicated, may hold values from -0.375 to 0.375
- conv_one: bfloat16 [1152, 128], replicated, may hold values from -0.1875 to 0.1875
- conv_two: bfloat16 [1152, 128], replicated, may hold values from -0.1875 to 0.1875
- kv_weight: bfloat16 [4096, 256], P('mp'), may hold values from -0.09375 to 0.09375
- w_query: bfloat16 [128, 128], replicated, may hold values from -0.5 to 0.5
- w_output: bfloat16 [128, 128], replicated, may hold values from -0.5 to 0.5
- w_head: bfloat16 [3, 128], replicated, may hold values from -0.5 to 0.5
Outputs:
- conv_one_update: float32 [1152, 128], P(('dp', 'mp'))
- conv_two_update: float32 [1152, 128], P(('dp', 'mp'))
- kv_update: float32 [4096, 256], P('mp', 'dp')
- loss_mean: float32 [], replicated
The draws below stay inside these ranges and needn't reach their ends.
All inputs are finite; a program needn't handle non-finite values.
Results may differ from the reference program's by a relative error of at most 0.03.
The reference program's roundings to bfloat16 on the way count: a program that leaves them out, or rounds other values in their place, can miss the bound.
Values may be sent and summed in bfloat16 or wider, within the bound.
A program may use at most 128 MiB of HBM per device.

```python
import math
import jax
import jax.numpy as jnp
from jax import lax

S = 64
C = 128
GROUPS = 32
HEADS = 2
HEAD_DIM = 64
A = 128
L = 128
DT = 4096
FREQS = 64
STEPS = 1000
BATCH = 256


def draw_text(key, part):
    base = jax.random.normal(jax.random.fold_in(key, 11), (BATCH, L, DT), jnp.float32)
    base = jnp.clip(base, -4.0, 4.0)
    return base.astype(jnp.bfloat16)


def draw_noise(key, part):
    ramp = jnp.arange(BATCH, dtype=jnp.float32) / max(BATCH - 1, 1)
    spread = (1.0 + 2.0 * ramp)[:, None, None]
    base = jnp.clip(jax.random.normal(jax.random.fold_in(key, 22), (BATCH, 3, S * S), jnp.float32), -4.0, 4.0)
    return (base * spread).astype(jnp.float32)


def set_ends(entries, stream_key, least, high):
    longest = entries.shape.index(max(entries.shape))
    spots = []
    for shift in (0, 1):
        where = [jax.random.randint(jax.random.fold_in(stream_key, axis), (), 0, length) for axis, length in enumerate(entries.shape)]
        where[longest] = (where[longest] + shift) % entries.shape[longest]
        spots.append(tuple(where))
    return entries.at[spots[0]].set(least).at[spots[1]].set(high)


def steps_of(rng, extent, cuts, low, largest):
    def one(axis_at, shards_of):
        steps = jax.random.uniform(jax.random.fold_in(jax.random.fold_in(rng, 6), axis_at), (shards_of,), jnp.float32, low / len(cuts), largest / len(cuts))
        return jnp.repeat(jnp.exp(steps), extent[axis_at] // shards_of).reshape((-1,) + (1,) * (len(extent) - axis_at - 1))

    gain = one(*cuts[0])
    for cut in cuts[1:]:
        gain = gain * one(*cut)
    return gain


def gaussian(stream_key, extent, scale, limit, cuts=(), kind=jnp.bfloat16):
    values = scale * jax.random.normal(stream_key, extent, jnp.float32)
    if cuts:
        values = values * steps_of(stream_key, extent, cuts, -0.22, 0.18)
    return jnp.clip(values, -limit, limit).astype(kind)


def setup_inputs(seed: int = 0) -> dict:
    arg_keys = jax.random.split(jax.random.key(seed), 17)
    clean = jnp.clip(jax.random.uniform(arg_keys[0], (BATCH, 3, S * S), jnp.float32, -1.0, 1.0) * steps_of(arg_keys[0], (BATCH, 3, S * S), ((0, 128),), -0.4, 0.0), -1.0, 1.0)
    noise = draw_noise(jax.random.fold_in(arg_keys[16], 71), 0)
    lowres = jnp.clip(jax.random.uniform(arg_keys[2], (BATCH, 3, S * S), jnp.float32, -1.0, 1.0) * steps_of(arg_keys[2], (BATCH, 3, S * S), ((0, 128),), -0.4, 0.0), -1.0, 1.0)
    aug_noise = gaussian(arg_keys[3], (BATCH, 3, S * S), 1.0, 5.0, ((0, 128),), jnp.float32)
    timesteps = set_ends(jax.random.randint(arg_keys[4], (BATCH,), 0, STEPS), jax.random.fold_in(arg_keys[4], 1), 0, STEPS - 1).astype(jnp.int32)
    aug_levels = set_ends(jax.random.randint(arg_keys[5], (BATCH,), 0, STEPS), jax.random.fold_in(arg_keys[5], 1), 0, STEPS - 1).astype(jnp.int32)
    lengths = set_ends(jax.random.randint(arg_keys[6], (BATCH,), 1, L + 1), jax.random.fold_in(arg_keys[6], 1), 1, L).astype(jnp.int32)
    text = draw_text(jax.random.fold_in(arg_keys[16], 71), 0)
    w_stem = gaussian(arg_keys[8], (6, C), 6 ** -0.5, 2.5, (), jnp.float32)
    w_time = gaussian(arg_keys[9], (4 * FREQS, 2 * C), (4 * FREQS) ** -0.5, 0.375, (), jnp.float32)
    conv_one = gaussian(arg_keys[10], (9 * C, C), (9 * C) ** -0.5, 0.1875)
    conv_two = gaussian(arg_keys[11], (9 * C, C), (9 * C) ** -0.5, 0.1875)
    kv_weight = gaussian(arg_keys[12], (DT, 2 * A), DT ** -0.5, 0.09375, ((0, 2),))
    w_query = gaussian(arg_keys[13], (C, A), C ** -0.5, 0.5)
    w_output = gaussian(arg_keys[14], (A, C), A ** -0.5, 0.5)
    w_head = gaussian(arg_keys[15], (3, C), C ** -0.5, 0.5)
    return dict(clean=clean, noise=noise, lowres=lowres, aug_noise=aug_noise, timesteps=timesteps, aug_levels=aug_levels, lengths=lengths, text=text, w_stem=w_stem, w_time=w_time, conv_one=conv_one, conv_two=conv_two, kv_weight=kv_weight, w_query=w_query, w_output=w_output, w_head=w_head)


def signal_level(index):
    ratio = (index.astype(jnp.float32) / STEPS + 0.008) / 1.008
    cosine = jnp.cos(ratio * (math.pi / 2.0))
    return cosine * cosine

def sinusoid(index):
    freqs = jnp.exp(-math.log(10000.0) * jnp.arange(FREQS, dtype=jnp.float32) / FREQS)
    angles = index.astype(jnp.float32) * freqs
    return jnp.concatenate([jnp.sin(angles), jnp.cos(angles)])

def prepare(clean, noise, lowres, aug_noise, tstep, level, w_stem, w_time):
    signal = signal_level(tstep)
    aug_signal = signal_level(level)
    noisy = jnp.sqrt(signal) * clean + jnp.sqrt(1.0 - signal) * noise
    low_noisy = jnp.sqrt(aug_signal) * lowres + jnp.sqrt(1.0 - aug_signal) * aug_noise
    stacked = jnp.concatenate([noisy, low_noisy], axis=0)
    h_start = jnp.einsum('kp,kc->pc', stacked, w_stem, precision=lax.Precision.HIGHEST)
    feature = jnp.concatenate([sinusoid(tstep), sinusoid(level)])[None, :]
    embed = jax.nn.silu(jnp.dot(feature, w_time, precision=lax.Precision.HIGHEST))[0]
    channels = w_stem.shape[1]
    return (h_start, embed[:channels], embed[channels:])

def group_matrix(channels):
    members = channels // GROUPS
    labels = jnp.arange(channels) // members
    return (labels[:, None] == labels[None, :]).astype(jnp.float32) / members

def group_norm(values, grouping):
    average = jnp.dot(lax.optimization_barrier(jnp.mean(values, axis=0, keepdims=True)), grouping, precision=lax.Precision.HIGHEST)
    centred = values - average
    spread = jnp.dot(lax.optimization_barrier(jnp.mean(centred * centred, axis=0, keepdims=True)), grouping, precision=lax.Precision.HIGHEST)
    return centred * lax.rsqrt(spread + 1e-05)

def convolve(activation, weight):
    channels = weight.shape[1]
    kernel = weight.reshape(3, 3, channels, channels)
    picture = activation.reshape(1, S, S, channels)
    result = lax.conv_general_dilated(picture, kernel, (1, 1), 'SAME', dimension_numbers=('NHWC', 'HWIO', 'NHWC'), preferred_element_type=jnp.float32)
    return result.reshape(S * S, channels)

def image_loss(conv_one, conv_two, keys_values, h_start, scale, shift, keep, w_query, w_output, w_head, noise):
    channels = conv_one.shape[1]
    grouping = group_matrix(channels)
    act_one = jax.nn.silu(group_norm(h_start, grouping)).astype(jnp.bfloat16)
    conv_out_one = convolve(act_one, conv_one)
    act_two = jax.nn.silu(group_norm(conv_out_one, grouping) * (1.0 + scale) + shift).astype(jnp.bfloat16)
    h_mid = h_start + convolve(act_two, conv_two)
    normed = group_norm(h_mid, grouping).astype(jnp.bfloat16)
    queries = (jnp.dot(normed, w_query, preferred_element_type=jnp.float32) * HEAD_DIM ** (-0.5)).astype(jnp.bfloat16)
    width = w_query.shape[1]
    pieces = []
    for head_index in range(HEADS):
        lower = head_index * HEAD_DIM
        upper = lower + HEAD_DIM
        scores = jnp.dot(queries[:, lower:upper], keys_values[:, lower:upper].T, preferred_element_type=jnp.float32)
        scores = jnp.where(keep[None, :], scores, -1e+30)
        highest = lax.optimization_barrier(jnp.max(scores, axis=1, keepdims=True))
        weights = jnp.exp(scores - highest)
        probs = (weights / lax.optimization_barrier(jnp.sum(weights, axis=1, keepdims=True))).astype(jnp.bfloat16)
        pieces.append(jnp.dot(probs, keys_values[:, width + lower:width + upper], preferred_element_type=jnp.float32))
    attended = jnp.concatenate(pieces, axis=1).astype(jnp.bfloat16)
    h_out = h_mid + jnp.dot(attended, w_output, preferred_element_type=jnp.float32)
    pred = jnp.einsum('kc,pc->kp', w_head.astype(jnp.float32), h_out.astype(jnp.bfloat16).astype(jnp.float32))
    error = pred - noise
    return jnp.sum(error * error)

def normalize(grad):
    return grad * lax.rsqrt(jnp.mean(grad * grad) + 1e-06)

def reference(clean, noise, lowres, aug_noise, timesteps, aug_levels, lengths, text, w_stem, w_time, conv_one, conv_two, kv_weight, w_query, w_output, w_head):

    def visit(carry, items):
        grad_one, grad_two, grad_kv, total = carry
        clean_i, noise_i, low_i, aug_i, tstep, level, length, text_i = items
        h_start, scale, shift = prepare(clean_i, noise_i, low_i, aug_i, tstep, level, w_stem, w_time)
        keys_values = jnp.dot(text_i, kv_weight, preferred_element_type=jnp.float32).astype(jnp.bfloat16)
        keep = jnp.arange(text_i.shape[0]).astype(jnp.int32) < length
        value, pullback = jax.vjp(lambda first, second, third: image_loss(first, second, third, h_start, scale, shift, keep, w_query, w_output, w_head, noise_i), conv_one, conv_two, keys_values)
        part_one, part_two, part_kv = pullback(jnp.ones((), value.dtype))
        grad_kv = grad_kv + jnp.dot(text_i.T, part_kv, preferred_element_type=jnp.float32)
        return ((grad_one + part_one.astype(jnp.float32), grad_two + part_two.astype(jnp.float32), grad_kv, total + value), None)
    start = (jnp.zeros(conv_one.shape, jnp.float32), jnp.zeros(conv_two.shape, jnp.float32), jnp.zeros(kv_weight.shape, jnp.float32), jnp.zeros((), jnp.float32))
    finals, unused = lax.scan(visit, start, (clean, noise, lowres, aug_noise, timesteps, aug_levels, lengths, text))
    grad_one, grad_two, grad_kv, total = finals
    count = clean.shape[0] * clean.shape[1] * clean.shape[2]
    return (normalize(grad_one), normalize(grad_two), normalize(grad_kv), total / count)
```

```python
import functools
import math

import jax
import jax.numpy as jnp
from jax import lax
from jax.sharding import Mesh
from jax.sharding import PartitionSpec as P
from jax.experimental import pallas as pl
from jax.experimental.pallas import tpu as pltpu

S = 64
GROUPS = 32
HEADS = 2
HEAD_DIM = 64
FREQS = 64
STEPS = 1000
DP_MP = ("dp_0", "dp_1", "dp_2", "dp_3", "mp")
DP = ("dp_0", "dp_1", "dp_2", "dp_3")


def in_order(tiles, dim):
    tiles = jnp.moveaxis(tiles, 0, dim)
    dims = tiles.shape
    return tiles.reshape(*dims[:dim], dims[dim] * dims[dim + 1], *dims[dim + 2 :])


def from_everyone(array, axis):
    copies = jnp.broadcast_to(array, (lax.axis_size(axis), *array.shape))
    return lax.all_to_all(copies, axis, split_axis=0, concat_axis=0, tiled=True)


def gather_directly(array, axis, dim):
    return in_order(from_everyone(array, axis), dim)


def split_up(array, dim, count):
    dims = array.shape
    tiles = array.reshape(*dims[:dim], count, dims[dim] // count, *dims[dim + 1 :])
    return jnp.moveaxis(tiles, dim, 0)


def sum_together(arrays, axis, dims):
    count = lax.axis_size(axis)
    tiles = [split_up(a, dim, count) for a, dim in zip(arrays, dims)]
    lines = jnp.concatenate([b.reshape(count, -1) for b in tiles], axis=1)
    width = max(16, -(-lines.shape[1] // 1024) * 8)
    lines = jnp.pad(lines, ((0, 0), (0, width * 128 - lines.shape[1]))).reshape(-1, 128)
    line, at, finished = (lax.psum_scatter(lines, axis, tiled=True).reshape(-1), 0, [])
    for b in tiles:
        part = b[0]
        finished.append(line[at : at + part.size].reshape(part.shape))
        at += part.size
    return tuple(finished)


def sent_and_summed(array, axis, dim):
    tiles = split_up(array, dim, lax.axis_size(axis))
    arrived = lax.all_to_all(tiles, axis, split_axis=0, concat_axis=0, tiled=True)
    return arrived.sum(axis=0)


def over_axes(array, axes):
    return functools.reduce(lax.psum, axes, array)


def signal_level(index):
    ratio = (index.astype(jnp.float32) / STEPS + 0.008) / 1.008
    cosine = jnp.cos(ratio * (math.pi / 2.0))
    return cosine * cosine


def sinusoid(index):
    freqs = jnp.exp(-math.log(10000.0) * jnp.arange(FREQS, dtype=jnp.float32) / FREQS)
    angles = index.astype(jnp.float32) * freqs
    return jnp.concatenate([jnp.sin(angles), jnp.cos(angles)])


def prepare(clean, noise, lowres, aug_noise, tstep, level, w_stem, w_time):
    signal = signal_level(tstep)
    aug_signal = signal_level(level)
    noisy = jnp.sqrt(signal) * clean + jnp.sqrt(1.0 - signal) * noise
    low_noisy = jnp.sqrt(aug_signal) * lowres + jnp.sqrt(1.0 - aug_signal) * aug_noise
    stacked = jnp.concatenate([noisy, low_noisy], axis=0)
    h_start = jnp.einsum("kp,kc->pc", stacked, w_stem, precision=lax.Precision.HIGHEST)
    feature = jnp.concatenate([sinusoid(tstep), sinusoid(level)])[None, :]
    embed = jax.nn.silu(jnp.dot(feature, w_time, precision=lax.Precision.HIGHEST))[0]
    channels = w_stem.shape[1]
    return (h_start, embed[:channels], embed[channels:])


def group_matrix(channels):
    members = channels // GROUPS
    labels = jnp.arange(channels) // members
    return (labels[:, None] == labels[None, :]).astype(jnp.float32) / members


def group_norm(values, grouping):
    average = jnp.dot(
        jnp.mean(values, axis=0, keepdims=True), grouping, precision=lax.Precision.HIGHEST
    )
    centred = values - average
    spread = jnp.dot(
        jnp.mean(centred * centred, axis=0, keepdims=True),
        grouping,
        precision=lax.Precision.HIGHEST,
    )
    return centred * lax.rsqrt(spread + 1e-05)


def convolve(activation, weight):
    channels = weight.shape[1]
    kernel = weight.reshape(3, 3, channels, channels)
    picture = activation.reshape(1, S, S, channels)
    result = lax.conv_general_dilated(
        picture,
        kernel,
        (1, 1),
        "SAME",
        dimension_numbers=("NHWC", "HWIO", "NHWC"),
        preferred_element_type=jnp.float32,
    )
    return result.reshape(S * S, channels)


def image_loss(
    conv_one, conv_two, keys_values, h_start, scale, shift, keep, w_query, w_output, w_head, noise
):
    channels = conv_one.shape[1]
    grouping = group_matrix(channels)
    act_one = jax.nn.silu(group_norm(h_start, grouping)).astype(jnp.bfloat16)
    conv_out_one = convolve(act_one, conv_one)
    act_two = jax.nn.silu(group_norm(conv_out_one, grouping) * (1.0 + scale) + shift).astype(
        jnp.bfloat16
    )
    h_mid = h_start + convolve(act_two, conv_two)
    normed = group_norm(h_mid, grouping).astype(jnp.bfloat16)
    queries = (
        jnp.dot(normed, w_query, preferred_element_type=jnp.float32) * HEAD_DIM ** (-0.5)
    ).astype(jnp.bfloat16)
    width = w_query.shape[1]
    pieces = []
    for head_index in range(HEADS):
        lower = head_index * HEAD_DIM
        upper = lower + HEAD_DIM
        scores = jnp.dot(
            queries[:, lower:upper],
            keys_values[:, lower:upper].T,
            preferred_element_type=jnp.float32,
        )
        scores = jnp.where(keep[None, :], scores, -1e30)
        highest = jnp.max(scores, axis=1, keepdims=True)
        weights = jnp.exp(scores - highest)
        probs = (weights / jnp.sum(weights, axis=1, keepdims=True)).astype(jnp.bfloat16)
        pieces.append(
            jnp.dot(
                probs,
                keys_values[:, width + lower : width + upper],
                preferred_element_type=jnp.float32,
            )
        )
    attended = jnp.concatenate(pieces, axis=1).astype(jnp.bfloat16)
    h_out = h_mid + jnp.dot(attended, w_output, preferred_element_type=jnp.float32)
    pred = jnp.einsum(
        "kc,pc->kp", w_head, h_out.astype(jnp.bfloat16), preferred_element_type=jnp.float32
    )
    error = pred - noise
    return jnp.sum(error * error)


AXES = ("dp_0", "dp_1", "dp_2", "dp_3", "mp")
MESH = pl.DeviceIdType.MESH
LINE = 4


def axis_target(axis, to):
    if axis == "x":
        return {"dp_1": to}
    if axis == "y":
        return {"dp_2": to}
    if axis == "z":
        return {"dp_0": to // 2, "mp": lax.rem(to, 2)}
    return {"dp_3": to}


ORDERS = (("x", "y", "z"), ("y", "z", "x"), ("z", "x", "y"))
DIMS = {0: ("x", "y", "z"), 1: None}


def part_of(ref, left, axis, at):
    index = tuple(at if name == axis else slice(None) for name in left)
    return ref.at[index]


def finish_kernel(
    counts,
    text_ref,
    cot_ref,
    conv_ref,
    loss_ref,
    one_ref,
    two_ref,
    kv_ref,
    mean_ref,
    rows_ref,
    wide_ref,
    own_a,
    own_b,
    core_in,
    held,
    line_in,
    second,
    second_in,
    third,
    third_in,
    total_ref,
    slots,
    send_sems,
    recv_sems,
    slot_send,
    slot_recv,
):
    place = {
        "x": lax.axis_index("dp_1"),
        "y": lax.axis_index("dp_2"),
        "z": lax.axis_index("dp_0") * 2 + lax.axis_index("mp"),
        "core": lax.axis_index("dp_3"),
    }
    core = place["core"]
    other = 1 - core
    barrier = pltpu.get_barrier_semaphore()
    pl.semaphore_signal(
        barrier, inc=1, device_id=axis_target("core", other), device_id_type=MESH
    )
    for axis in ("x", "y", "z"):
        for k in range(1, LINE):
            to = lax.rem(place[axis] + k, LINE)
            pl.semaphore_signal(
                barrier, inc=1, device_id=axis_target(axis, to), device_id_type=MESH
            )

    tokens = cot_ref.shape[0]
    for q in range(4):
        row = lax.broadcasted_iota(jnp.int32, (1024, 256), 0)
        col = lax.broadcasted_iota(jnp.int32, (1024, 256), 1)
        j = row % 4
        qq = (row // 4) % 4
        zh = (row // 16) % 2
        y = (row // 32) % 4
        x = (row // 128) % 4
        c = row // 512
        source = (((zh * 4 + x) * 4 + y) * 2 + c) * 4 + j
        pick = jnp.where((source == col) & (qq == q), 1.0, 0.0).astype(jnp.bfloat16)
        rows_ref[:, q * tokens : (q + 1) * tokens] = lax.dot_general(
            pick,
            cot_ref[...],
            (((1,), (1,)), ((), ())),
            preferred_element_type=jnp.float32,
        ).astype(jnp.bfloat16)
        for m in range(2):
            wide_ref[q * tokens : (q + 1) * tokens, m * 512 : (m + 1) * 512] = text_ref[
                :, m * 2048 + q * 512 : m * 2048 + (q + 1) * 512
            ]

    def block(i, carry):
        rows = rows_ref[pl.ds(pl.multiple_of(i * 128, 128), 128), :]
        for m in range(2):
            value = jnp.dot(
                rows, wide_ref[:, m * 512 : (m + 1) * 512], preferred_element_type=jnp.float32
            ).astype(jnp.bfloat16)
            value = value.reshape(4, 2, 16, 512)
            at = lax.rem(i, 4)
            for zh in range(2):
                own_a[i // 4, at, :, zh * 2 + m] = value[:, zh, :, :256]
                own_b[i // 4, at, :, zh * 2 + m] = value[:, zh, :, 256:]
        return carry

    lax.fori_loop(0, 8, block, 0)

    pl.semaphore_wait(barrier, 10)

    firsts = (own_a, own_b, conv_ref)
    copies = []
    for c in range(3):
        copy = pltpu.make_async_remote_copy(
            src_ref=firsts[c].at[other],
            dst_ref=core_in.at[c],
            send_sem=send_sems.at[c],
            recv_sem=recv_sems.at[c],
            device_id=axis_target("core", other),
            device_id_type=MESH,
        )
        copy.start()
        copies.append(copy)

    def exchange(c, stage, source, left, into):
        axis = ORDERS[c][stage]
        started = []
        for k in range(1, LINE):
            to = lax.rem(place[axis] + k, LINE)
            slot = 3 + (c * 3 + stage) * 3 + k - 1
            copy = pltpu.make_async_remote_copy(
                src_ref=part_of(source.at[c], left, axis, to),
                dst_ref=into.at[c, k - 1],
                send_sem=send_sems.at[slot],
                recv_sem=recv_sems.at[slot],
                device_id=axis_target(axis, to),
                device_id_type=MESH,
            )
            copy.start()
            started.append(copy)
        return started

    lines = []
    for c in range(3):
        copies[c].wait_recv()

        def add(i, carry, c=c):
            held[c, i] = (
                firsts[c][core, i].astype(jnp.float32) + core_in[c, i].astype(jnp.float32)
            ).astype(jnp.bfloat16)
            return carry

        lax.fori_loop(0, LINE, add, 0)
        lines.append(exchange(c, 0, held, ("x", "y", "z"), line_in))

    def own_part(ref, c, left, axis):
        index = tuple(place[axis] if name == axis else slice(None) for name in left)
        return ref[(c,) + index]

    seconds = []
    for c in range(3):
        axis = ORDERS[c][0]
        for copy in lines[c]:
            copy.wait_recv()
        for i in range(LINE):
            rest = [name for name in ("x", "y", "z") if name != axis]
            index = tuple(
                place[axis] if name == axis else (i if name == rest[0] else slice(None))
                for name in ("x", "y", "z")
            )
            value = held[(c,) + index].astype(jnp.float32)
            for k in range(LINE - 1):
                value = value + line_in[c, k, i].astype(jnp.float32)
            second[c, i] = value.astype(jnp.bfloat16)
        left = tuple(name for name in ("x", "y", "z") if name != axis)
        seconds.append(exchange(c, 1, second, left, second_in))

    thirds = []
    for c in range(3):
        left = tuple(name for name in ("x", "y", "z") if name != ORDERS[c][0])
        axis = ORDERS[c][1]
        for copy in seconds[c]:
            copy.wait_recv()
        value = own_part(second, c, left, axis).astype(jnp.float32)
        for k in range(LINE - 1):
            value = value + second_in[c, k].astype(jnp.float32)
        third[c] = value.astype(jnp.bfloat16)
        thirds.append(exchange(c, 2, third, (ORDERS[c][2],), third_in))

    for c in range(3):
        axis = ORDERS[c][2]
        for copy in thirds[c]:
            copy.wait_recv()
        value = third[c, place[axis]].astype(jnp.float32)
        for k in range(LINE - 1):
            value = value + third_in[c, k].astype(jnp.float32)
        total_ref[:, c * 256 : (c + 1) * 256] = value

    value = total_ref[...]
    square = value * value
    kv_line = jnp.sum(square[:, :512], axis=0, keepdims=True)
    kv_line = (
        kv_line[:, :128] + kv_line[:, 128:256] + kv_line[:, 256:384] + kv_line[:, 384:512]
    )
    conv_line = jnp.sum(square[:, 512:], axis=0, keepdims=True)
    row = lax.broadcasted_iota(jnp.int32, (8, 128), 0)
    tile = jnp.where(row == 0, kv_line, 0.0)
    tile = jnp.where(row == 1, conv_line[:, :128], tile)
    tile = jnp.where(row == 2, conv_line[:, 128:], tile)
    tile = jnp.where(row == 3, loss_ref[...], tile)
    at = 0
    for stage, axis in enumerate(("core", "x", "y", "z")):
        size = 2 if axis == "core" else LINE
        slots[stage, place[axis]] = tile
        started = []
        for k in range(1, size):
            to = lax.rem(place[axis] + k, size)
            copy = pltpu.make_async_remote_copy(
                src_ref=slots.at[stage, place[axis]],
                dst_ref=slots.at[stage, place[axis]],
                send_sem=slot_send.at[at],
                recv_sem=slot_recv.at[at],
                device_id=axis_target(axis, to),
                device_id_type=MESH,
            )
            copy.start()
            started.append(copy)
            at += 1
        for copy in started:
            copy.wait_recv()
        tile = slots[stage, 0]
        for k in range(1, size):
            tile = tile + slots[stage, k]
        for copy in started:
            copy.wait_send()
    sums = jnp.sum(tile, axis=1, keepdims=True)
    kv_scale = lax.rsqrt(sums[0:1] / counts[0] + 1e-06)
    one_scale = lax.rsqrt(sums[1:2] / counts[1] + 1e-06)
    two_scale = lax.rsqrt(sums[2:3] / counts[1] + 1e-06)
    one_ref[...] = total_ref[0:9, 512:640] * one_scale
    two_ref[...] = total_ref[0:9, 640:768] * two_scale
    for q in range(4):
        kv_ref[:, q * 512 : (q + 1) * 512] = total_ref[q * 4 : (q + 1) * 4, 0:512] * kv_scale
    mean_ref[...] = jnp.broadcast_to(sums[3:4] / counts[2], mean_ref.shape)
    for copy in copies:
        copy.wait_send()
    for group in lines + seconds + thirds:
        for copy in group:
            copy.wait_send()


def finish(text, cot, conv, loss, counts):
    bf16, f32 = jnp.bfloat16, jnp.float32
    return pl.pallas_call(
        functools.partial(finish_kernel, counts),
        out_shape=(
            jax.ShapeDtypeStruct((9, 128), f32),
            jax.ShapeDtypeStruct((9, 128), f32),
            jax.ShapeDtypeStruct((4, 2048), f32),
            jax.ShapeDtypeStruct((1, 128), f32),
        ),
        in_specs=[pl.BlockSpec(memory_space=pltpu.VMEM)] * 4,
        out_specs=[pl.BlockSpec(memory_space=pltpu.VMEM)] * 4,
        scratch_shapes=[
            pltpu.VMEM((1024, 1024), bf16),
            pltpu.VMEM((1024, 1024), bf16),
            pltpu.VMEM((2, 4, 4, 4, 16, 256), bf16),
            pltpu.VMEM((2, 4, 4, 4, 16, 256), bf16),
            pltpu.VMEM((3, 4, 4, 4, 16, 256), bf16),
            pltpu.VMEM((3, 4, 4, 4, 16, 256), bf16),
            pltpu.VMEM((3, 3, 4, 4, 16, 256), bf16),
            pltpu.VMEM((3, 4, 4, 16, 256), bf16),
            pltpu.VMEM((3, 3, 4, 16, 256), bf16),
            pltpu.VMEM((3, 4, 16, 256), bf16),
            pltpu.VMEM((3, 3, 16, 256), bf16),
            pltpu.VMEM((16, 768), f32),
            pltpu.VMEM((4, 4, 8, 128), f32),
            pltpu.SemaphoreType.DMA((30,)),
            pltpu.SemaphoreType.DMA((30,)),
            pltpu.SemaphoreType.DMA((10,)),
            pltpu.SemaphoreType.DMA((10,)),
        ],
        compiler_params=pltpu.CompilerParams(
            collective_id=0, has_side_effects=True, vmem_limit_bytes=40 * 2**20
        ),
        cost_estimate=pl.CostEstimate(
            flops=3 * 10**9, bytes_accessed=8 * 10**6, transcendentals=0
        ),
        name="finish",
    )(text, cot, conv, loss)


def by_owner(grad):
    tiles = grad.reshape(2, 4, 4, 2, 2, 9, 128)
    tiles = jnp.transpose(tiles, (3, 1, 2, 0, 4, 5, 6)).reshape(2, 4, 4, 4, 9, 128)
    return jnp.pad(tiles, ((0, 0),) * 4 + ((0, 7), (0, 0))).astype(jnp.bfloat16)


def local(
    clean,
    noise,
    lowres,
    aug_noise,
    timesteps,
    aug_levels,
    lengths,
    text,
    w_stem,
    w_time,
    conv_one,
    conv_two,
    kv_weight,
    w_query,
    w_output,
    w_head,
):
    images = clean.shape[0]
    tokens = text.shape[1]
    features = text.shape[2]
    width = kv_weight.shape[1]
    half = kv_weight.shape[0]
    piece = gather_directly(kv_weight, "mp", 0)
    flat = jnp.dot(
        text.reshape(images * tokens, piece.shape[0]), piece, preferred_element_type=jnp.float32
    )
    summed = flat.reshape(images, tokens, width)
    keys_values = summed.astype(jnp.bfloat16)

    def one_image(items):
        clean_i, noise_i, low_i, aug_i, tstep, level, length, pairs = items
        h_start, scale, shift = prepare(
            clean_i, noise_i, low_i, aug_i, tstep, level, w_stem, w_time
        )
        keep = jnp.arange(tokens) < length
        value, pullback = jax.vjp(
            lambda first, second, third: image_loss(
                first,
                second,
                third,
                h_start,
                scale,
                shift,
                keep,
                w_query,
                w_output,
                w_head,
                noise_i,
            ),
            conv_one,
            conv_two,
            pairs,
        )
        part_one, part_two, part_kv = pullback(jnp.ones((), jnp.float32))
        return (part_one, part_two, part_kv, value)

    parts_one, parts_two, parts_kv, values = lax.map(
        one_image, (clean, noise, lowres, aug_noise, timesteps, aug_levels, lengths, keys_values)
    )
    local_one = jnp.sum(parts_one.astype(jnp.float32), axis=0)
    local_two = jnp.sum(parts_two.astype(jnp.float32), axis=0)
    local_loss = jnp.sum(values)
    conv = jnp.concatenate([by_owner(local_one), by_owner(local_two)], axis=-1)
    counts = (
        2 * half * width,
        conv_one.shape[0] * conv_one.shape[1],
        images * lax.axis_size(DP_MP) * clean.shape[1] * clean.shape[2],
    )
    lane = lax.broadcasted_iota(jnp.int32, (1, 128), 1)
    loss = jnp.where(lane == 0, local_loss, 0.0)
    conv_one_update, conv_two_update, kv, mean = finish(
        text.reshape(-1, features), parts_kv.reshape(-1, width), conv, loss, counts
    )
    return (conv_one_update, conv_two_update, kv.T, mean[0, 0])


def solution(mesh):
    finer = Mesh(
        mesh.devices.reshape(2, 4, 4, 2, mesh.shape["mp"]), ("dp_0", "dp_1", "dp_2", "dp_3", "mp")
    )
    placed = (
        P(DP_MP, None, None),
        P(DP_MP, None, None),
        P(DP_MP, None, None),
        P(DP_MP, None, None),
        P(DP_MP),
        P(DP_MP),
        P(DP_MP),
        P(DP_MP, None, None),
        P(),
        P(),
        P(),
        P(),
        P("mp", None),
        P(),
        P(),
        P(),
    )
    return jax.shard_map(
        local,
        mesh=finer,
        in_specs=placed,
        out_specs=(P(DP_MP, None), P(DP_MP, None), P("mp", DP), P()),
        check_vma=False,
    )
```

```python
import functools
import math

import jax
import jax.numpy as jnp
import numpy as np
from jax import lax
from jax.sharding import Mesh
from jax.sharding import PartitionSpec as P
from jax.experimental import pallas as pl
from jax.experimental.pallas import tpu as pltpu

S = 64
GROUPS = 32
HEADS = 2
HEAD_DIM = 64
FREQS = 64
STEPS = 1000
DP_MP = ("dp_0", "dp_1", "dp_2", "dp_3", "mp")
DP = ("dp_0", "dp_1", "dp_2", "dp_3")


def signal_level(index):
    ratio = (index.astype(jnp.float32) / STEPS + 0.008) / 1.008
    cosine = jnp.cos(ratio * (math.pi / 2.0))
    return cosine * cosine


PIXELS = S * S
CHUNK = 512
CHUNKS = PIXELS // CHUNK
EDGE = S
C = 128


def group_total(line):
    lane = lax.broadcasted_iota(jnp.int32, line.shape, 1)
    pair = line + jnp.where(
        lane % 2 == 0, pltpu.roll(line, C - 1, 1), pltpu.roll(line, 1, 1)
    )
    return pair + jnp.where(
        lane % 4 < 2, pltpu.roll(pair, C - 2, 1), pltpu.roll(pair, 2, 1)
    )


def group_mean(total):
    line = jnp.broadcast_to(jnp.sum(total, axis=0, keepdims=True), (8, C)) / PIXELS
    return group_total(line)[0:1] / (C // GROUPS)


def row_of(value, i):
    row = value[0:1]
    for r in range(1, value.shape[0]):
        row = jnp.where(i == r, value[r : r + 1], row)
    return row


def fold(value):
    return jnp.sum(value.reshape(-1, 8, value.shape[-1]), axis=0)


def spread(act):
    column = lax.broadcasted_iota(jnp.int32, act.shape, 0) % S
    rows = act.shape[0]
    left = jnp.where(column == 0, 0.0, pltpu.roll(act, 1, 0))
    right = jnp.where(column == S - 1, 0.0, pltpu.roll(act, rows - 1, 0))
    return jnp.concatenate(
        [left.astype(jnp.bfloat16), act.astype(jnp.bfloat16), right.astype(jnp.bfloat16)], axis=1
    )


def span(j, size=CHUNK):
    return pl.ds(pl.multiple_of(j * size, size), size)


def shifted(j, dy, size=CHUNK):
    return pl.ds(pl.multiple_of(j * size + dy * S, S), size)


def clear_edges(ref, i):
    zero = jnp.zeros((EDGE, 3 * C), jnp.bfloat16)
    ref[i, :EDGE] = zero
    ref[i, EDGE + PIXELS :] = zero


def conv_rows(wide_ref, i, j, weight_ref):
    rows = jnp.concatenate([wide_ref[i, shifted(j, dy)] for dy in range(3)], axis=1)
    return jnp.dot(rows, weight_ref[...], preferred_element_type=jnp.float32)


def loop_sum(body, width=C):
    return lax.fori_loop(0, CHUNKS, body, jnp.zeros((8, width), jnp.float32))


def forward_kernel(
    coef_ref,
    clean_ref,
    noise_ref,
    low_ref,
    aug_ref,
    stem_ref,
    feature_ref,
    time_ref,
    one_ref,
    two_ref,
    mid_ref,
    out_ref,
    wide_one,
    wide_two,
    stats_ref,
    planes_ref,
    stems_ref,
    embed_ref,
    lhs_ref,
):
    images = clean_ref.shape[1]
    w = jnp.concatenate([stem_ref[...], jnp.zeros((2, C), jnp.float32)], axis=0)
    w1 = w.astype(jnp.bfloat16).astype(jnp.float32)
    w2 = (w - w1).astype(jnp.bfloat16).astype(jnp.float32)
    w3 = w - w1 - w2
    stems_ref[...] = jnp.concatenate([w1, w2, w1, w3, w2, w1], axis=0).astype(jnp.bfloat16)
    feature = jnp.concatenate(
        [feature_ref[...], jnp.zeros((8 - images, 2 * C), jnp.float32)], axis=0
    )
    embed = jnp.dot(
        feature,
        time_ref[...],
        precision=lax.Precision.HIGHEST,
        preferred_element_type=jnp.float32,
    )
    embed_ref[...] = embed * jax.nn.sigmoid(embed)
    planes_ref[...] = jnp.zeros(planes_ref.shape, jnp.float32)

    def image(i, carry):
        for k in range(3):
            planes_ref[k : k + 1] = (
                coef_ref[i, 0] * row_of(clean_ref[k], i)
                + coef_ref[i, 1] * row_of(noise_ref[k], i)
            )
            planes_ref[3 + k : 4 + k] = (
                coef_ref[i, 2] * row_of(low_ref[k], i) + coef_ref[i, 3] * row_of(aug_ref[k], i)
            )
        s = planes_ref[...]
        s1 = s.astype(jnp.bfloat16).astype(jnp.float32)
        s2 = (s - s1).astype(jnp.bfloat16).astype(jnp.float32)
        s3 = s - s1 - s2
        lhs_ref[...] = jnp.concatenate([s1, s1, s2, s1, s2, s3], axis=0).astype(jnp.bfloat16)
        clear_edges(wide_one, i)
        clear_edges(wide_two, i)

        def stem(j, total):
            h = lax.dot_general(
                lhs_ref[:, span(j)],
                stems_ref[...],
                (((0,), (0,)), ((), ())),
                preferred_element_type=jnp.float32,
            )
            mid_ref[i, span(j)] = h
            return total + fold(h)

        def variance(ref, mean):
            def body(j, total):
                centred = ref[i, span(j)] - mean
                return total + fold(centred * centred)

            return lax.rsqrt(group_mean(loop_sum(body)) + 1e-05)

        mean_one = group_mean(loop_sum(stem))
        inv_one = variance(mid_ref, mean_one)

        def first(j, carry):
            act = (mid_ref[i, span(j)] - mean_one) * inv_one
            wide_one[i, shifted(j, 1)] = spread(act * jax.nn.sigmoid(act))
            return carry

        lax.fori_loop(0, CHUNKS, first, 0)

        def conv_first(j, total):
            value = conv_rows(wide_one, i, j, one_ref)
            out_ref[i, span(j)] = value
            return total + fold(value)

        mean_two = group_mean(loop_sum(conv_first))
        inv_two = variance(out_ref, mean_two)
        gain = 1.0 + row_of(embed_ref[0:images, 0:C], i)
        shift = row_of(embed_ref[0:images, C : 2 * C], i)

        def next_act(j, carry):
            act = (out_ref[i, span(j)] - mean_two) * inv_two * gain + shift
            wide_two[i, shifted(j, 1)] = spread(act * jax.nn.sigmoid(act))
            return carry

        lax.fori_loop(0, CHUNKS, next_act, 0)

        def conv_second(j, total):
            value = mid_ref[i, span(j)] + conv_rows(wide_two, i, j, two_ref)
            mid_ref[i, span(j)] = value
            return total + fold(value)

        mean_three = group_mean(loop_sum(conv_second))
        inv_three = variance(mid_ref, mean_three)
        stats_ref[i] = jnp.concatenate(
            [mean_two, inv_two, mean_three, inv_three, gain, shift, gain, shift], axis=0
        )
        return carry

    lax.fori_loop(0, images, image, 0)


def forward(coefs, clean, noise, lowres, aug_noise, stem, feature, w_time, conv_one, conv_two):
    images = clean.shape[1]
    bf16, f32 = jnp.bfloat16, jnp.float32
    wide = jax.ShapeDtypeStruct((images, PIXELS + 2 * EDGE, 3 * C), bf16)
    flat = jax.ShapeDtypeStruct((images, PIXELS, C), f32)
    return pl.pallas_call(
        forward_kernel,
        out_shape=(flat, flat, wide, wide, jax.ShapeDtypeStruct((images, 8, C), f32)),
        in_specs=[pl.BlockSpec(memory_space=pltpu.SMEM)]
        + [pl.BlockSpec(memory_space=pltpu.VMEM)] * 9,
        out_specs=[pl.BlockSpec(memory_space=pltpu.VMEM)] * 5,
        scratch_shapes=[
            pltpu.VMEM((8, PIXELS), f32),
            pltpu.VMEM((48, C), bf16),
            pltpu.VMEM((8, 2 * C), f32),
            pltpu.VMEM((48, PIXELS), bf16),
        ],
        compiler_params=pltpu.CompilerParams(vmem_limit_bytes=LIMIT_F * 2**20),
        cost_estimate=pl.CostEstimate(
            flops=10**10, bytes_accessed=22 * 10**6, transcendentals=2 * 10**6
        ),
        name="forward",
    )(coefs, clean, noise, lowres, aug_noise, stem, feature, w_time, conv_one, conv_two)


TN = (((0,), (0,)), ((), ()))
NT = (((1,), (1,)), ((), ()))


def mm(a, b, dims=(((1,), (0,)), ((), ()))):
    return lax.dot_general(a, b, dims, preferred_element_type=jnp.float32)


def backward_kernel(
    half_ref,
    lengths_ref,
    noise_ref,
    text_ref,
    near_ref,
    far_ref,
    mid_ref,
    out_ref,
    wide_one,
    wide_two,
    stats_ref,
    two_ref,
    query_ref,
    output_ref,
    heads_ref,
    cot_ref,
    conv_ref,
    loss_ref,
    kv_ref,
    key_ref,
    val_ref,
    dkey_ref,
    dval_ref,
    dnorm_ref,
    dout_ref,
    dhat_ref,
    wide_grad,
    grad_ref,
    flat_ref,
    total_ref,
    flip_ref,
    head_ref,
    goal_ref,
):
    bf16, f32 = jnp.bfloat16, jnp.float32
    images = noise_ref.shape[1]
    tokens = text_ref.shape[0] // images
    half = near_ref.shape[0]
    mp = half_ref[0]
    here = pl.ds(pl.multiple_of(mp * half, half), half)
    there = pl.ds(pl.multiple_of((1 - mp) * half, half), half)
    kv_ref[...] = (
        mm(text_ref[:, here], near_ref[...]) + mm(text_ref[:, there], far_ref[...])
    ).astype(bf16)
    total_ref[...] = jnp.zeros(total_ref.shape, f32)
    clear_edges(wide_grad, 0)
    for tap in range(9):
        flip_ref[(8 - tap) * C : (9 - tap) * C] = two_ref[tap * C : (tap + 1) * C].T
    head_ref[...] = jnp.concatenate(
        [heads_ref[...].astype(f32), jnp.zeros((8 - heads_ref.shape[0], C), f32)], axis=0
    ).astype(bf16)
    goal_ref[...] = jnp.zeros(goal_ref.shape, f32)
    lane = lax.broadcasted_iota(jnp.int32, (tokens, C), 1)

    def image(i, loss):
        for k in range(3):
            goal_ref[k : k + 1] = row_of(noise_ref[k], i)
        both = kv_ref[pl.ds(pl.multiple_of(i * tokens, tokens), tokens), :]
        zero = jnp.zeros((tokens, C), bf16)
        low = lane < HEAD_DIM
        key_ref[...] = jnp.concatenate(
            [jnp.where(low, both[:, :C], zero), jnp.where(low, zero, both[:, :C])], axis=0
        )
        val_ref[...] = jnp.concatenate(
            [jnp.where(low, both[:, C:], zero), jnp.where(low, zero, both[:, C:])], axis=0
        )
        dkey_ref[...] = jnp.zeros(dkey_ref.shape, f32)
        dval_ref[...] = jnp.zeros(dval_ref.shape, f32)
        mean_two, inv_two = stats_ref[i, 0:1], stats_ref[i, 1:2]
        mean_three, inv_three = stats_ref[i, 2:3], stats_ref[i, 3:4]
        gain, shift = stats_ref[i, 4:5], stats_ref[i, 5:6]
        keep = lax.broadcasted_iota(jnp.int32, (CHUNK, tokens), 1) < lengths_ref[i]

        def attend(j, carry):
            total, moment, loss = carry
            mid = mid_ref[i, span(j)]
            hat = (mid - mean_three) * inv_three
            query = (mm(hat.astype(bf16), query_ref[...]) * HEAD_DIM ** (-0.5)).astype(bf16)
            scores = mm(query, key_ref[...], NT)
            probs = []
            for h in range(HEADS):
                one = jnp.where(keep, scores[:, h * tokens : (h + 1) * tokens], -1e30)
                one = jnp.exp(one - jnp.max(one, axis=1, keepdims=True))
                probs.append(one / jnp.sum(one, axis=1, keepdims=True))
            rounded = jnp.concatenate([p.astype(bf16) for p in probs], axis=1)
            attended = mm(rounded, val_ref[...]).astype(bf16)
            out = (mid + mm(attended, output_ref[...])).astype(bf16)
            pred = mm(out, head_ref[...], NT)
            error = pred - goal_ref[:, span(j)].T
            loss = loss + fold(error * error)
            dout = mm((2.0 * error).astype(bf16), head_ref[...]).astype(bf16)
            dout_ref[span(j)] = dout
            datt = mm(dout, output_ref[...], NT).astype(bf16)
            dprobs = mm(datt, val_ref[...], NT).astype(bf16).astype(f32)
            dval_ref[...] += mm(datt, rounded, TN)
            dscores = []
            for h in range(HEADS):
                one = dprobs[:, h * tokens : (h + 1) * tokens]
                inner = jnp.sum(one * probs[h], axis=1, keepdims=True)
                dscores.append((probs[h] * (one - inner)).astype(bf16))
            dscores = jnp.concatenate(dscores, axis=1)
            dkey_ref[...] += mm(query, dscores, TN)
            dquery = mm(dscores, key_ref[...]).astype(bf16)
            dnorm = (mm(dquery, query_ref[...], NT) * HEAD_DIM ** (-0.5)).astype(bf16)
            dnorm_ref[span(j)] = dnorm
            dnorm = dnorm.astype(f32)
            return (total + fold(dnorm), moment + fold(dnorm * hat), loss)

        nothing = jnp.zeros((8, C), f32)
        total, moment, loss = lax.fori_loop(0, CHUNKS, attend, (nothing, nothing, loss))
        low_row = lax.broadcasted_iota(jnp.int32, (C, tokens), 0) < HEAD_DIM
        cots = [
            jnp.where(low_row, ref[:, :tokens], ref[:, tokens:]) for ref in (dkey_ref, dval_ref)
        ]
        cot_ref[:, pl.ds(pl.multiple_of(i * tokens, tokens), tokens)] = jnp.concatenate(
            cots, axis=0
        ).astype(bf16)
        first, second = group_mean(total), group_mean(moment)

        def middle(j, carry):
            hat = (mid_ref[i, span(j)] - mean_three) * inv_three
            grad = dout_ref[span(j)].astype(f32) + inv_three * (
                dnorm_ref[span(j)].astype(f32) - first - hat * second
            )
            wide_grad[0, shifted(j, 1)] = spread(grad)
            return carry

        lax.fori_loop(0, CHUNKS, middle, 0)

        def weights(which, source, grads):
            grad_ref[...] = jnp.zeros(grad_ref.shape, f32)

            def body(j, carry):
                grad = grads(j)
                for dy in range(3):
                    grad_ref[:, dy * 3 * C : (dy + 1) * 3 * C] += mm(
                        grad, source[i, shifted(j, dy)], TN
                    )
                return carry

            lax.fori_loop(0, CHUNKS, body, 0)
            total_ref[which] += grad_ref[...].astype(bf16).astype(f32)

        weights(1, wide_two, lambda j: wide_grad[0, shifted(j, 1), C : 2 * C])

        def inner(j, carry):
            total, moment = carry
            dact = conv_rows(wide_grad, 0, j, flip_ref).astype(bf16).astype(f32)
            hat = (out_ref[i, span(j)] - mean_two) * inv_two
            act = hat * gain + shift
            gate = jax.nn.sigmoid(act)
            dhat = dact * (gate * (1.0 + act * (1.0 - gate))) * gain
            dhat_ref[span(j)] = dhat
            return (total + fold(dhat), moment + fold(dhat * hat))

        total, moment = lax.fori_loop(0, CHUNKS, inner, (nothing, nothing))
        first, second = group_mean(total), group_mean(moment)

        def early(j):
            hat = (out_ref[i, span(j)] - mean_two) * inv_two
            return (inv_two * (dhat_ref[span(j)] - first - hat * second)).astype(bf16)

        weights(0, wide_one, early)
        return loss

    loss = lax.fori_loop(0, images, image, jnp.zeros((8, 8), f32))
    loss_ref[...] = jnp.broadcast_to(
        jnp.sum(jnp.sum(loss, axis=0, keepdims=True), axis=1, keepdims=True) / C, (1, C)
    )
    for which in range(2):
        for block in range(9):
            flat_ref[which, block * C : (block + 1) * C] = total_ref[
                which, :, block * C : (block + 1) * C
            ].T
    flat_ref[:, 9 * C :] = jnp.zeros((2, 16, C), f32)
    row = lax.broadcasted_iota(jnp.int32, (16, C), 0)

    def owner(d, carry):
        pieces = [
            jnp.where(row < 9, flat_ref[which, pl.ds(d * 9, 16)], 0.0).astype(bf16)
            for which in range(2)
        ]
        low = lax.rem(d, 2)
        core = lax.rem(d // 2, 2)
        y = lax.rem(d // 4, 4)
        x = lax.rem(d // 16, 4)
        high = d // 64
        conv_ref[core, x, y, high * 2 + low] = jnp.concatenate(pieces, axis=1)
        return carry

    lax.fori_loop(0, 128, owner, 0)


def backward(half, lengths, noise, text, near, far, made, conv_two, w_query, w_output, head):
    images = noise.shape[1]
    bf16, f32 = jnp.bfloat16, jnp.float32
    tokens = text.shape[0] // images
    vmem = pl.BlockSpec(memory_space=pltpu.VMEM)
    smem = pl.BlockSpec(memory_space=pltpu.SMEM)
    return pl.pallas_call(
        backward_kernel,
        out_shape=(
            jax.ShapeDtypeStruct((2 * C, images * tokens), bf16),
            jax.ShapeDtypeStruct((2, 4, 4, 4, 16, 2 * C), bf16),
            jax.ShapeDtypeStruct((1, C), f32),
        ),
        in_specs=[smem] * 2 + [vmem] * 13,
        out_specs=[vmem] * 3,
        scratch_shapes=[
            pltpu.VMEM((images * tokens, 2 * C), bf16),
            pltpu.VMEM((2 * tokens, C), bf16),
            pltpu.VMEM((2 * tokens, C), bf16),
            pltpu.VMEM((C, 2 * tokens), f32),
            pltpu.VMEM((C, 2 * tokens), f32),
            pltpu.VMEM((PIXELS, C), bf16),
            pltpu.VMEM((PIXELS, C), bf16),
            pltpu.VMEM((PIXELS, C), f32),
            pltpu.VMEM((1, PIXELS + 2 * EDGE, 3 * C), bf16),
            pltpu.VMEM((C, 9 * C), f32),
            pltpu.VMEM((2, 9 * C + 16, C), f32),
            pltpu.VMEM((2, C, 9 * C), f32),
            pltpu.VMEM((9 * C, C), bf16),
            pltpu.VMEM((8, C), bf16),
            pltpu.VMEM((8, PIXELS), f32),
        ],
        compiler_params=pltpu.CompilerParams(vmem_limit_bytes=LIMIT_B * 2**20),
        cost_estimate=pl.CostEstimate(
            flops=2 * 10**10, bytes_accessed=26 * 10**6, transcendentals=6 * 10**6
        ),
        name="backward",
    )(half, lengths, noise, text, near, far, *made, conv_two, w_query, w_output, head)


LIMIT_F = 8
LIMIT_B = 20


AXES = ("dp_0", "dp_1", "dp_2", "dp_3", "mp")
MESH = pl.DeviceIdType.MESH
LINE = 4


def axis_target(axis, to):
    if axis == "x":
        return {"dp_1": to}
    if axis == "y":
        return {"dp_2": to}
    if axis == "z":
        return {"dp_0": to // 2, "mp": lax.rem(to, 2)}
    return {"dp_3": to}


ORDERS = (("x", "y", "z"), ("y", "z", "x"), ("z", "x", "y"))
DIMS = {0: ("x", "y", "z"), 1: None}


def part_of(ref, left, axis, at):
    index = tuple(at if name == axis else slice(None) for name in left)
    return ref.at[index]


def finish_kernel(
    counts,
    text_ref,
    cot_ref,
    conv_ref,
    loss_ref,
    one_ref,
    two_ref,
    kv_ref,
    mean_ref,
    rows_ref,
    wide_ref,
    own_a,
    own_b,
    core_in,
    held,
    line_in,
    second,
    second_in,
    third,
    third_in,
    total_ref,
    slots,
    send_sems,
    recv_sems,
    slot_send,
    slot_recv,
):
    place = {
        "x": lax.axis_index("dp_1"),
        "y": lax.axis_index("dp_2"),
        "z": lax.axis_index("dp_0") * 2 + lax.axis_index("mp"),
        "core": lax.axis_index("dp_3"),
    }
    core = place["core"]
    other = 1 - core
    barrier = pltpu.get_barrier_semaphore()
    pl.semaphore_signal(
        barrier, inc=1, device_id=axis_target("core", other), device_id_type=MESH
    )
    for axis in ("x", "y", "z"):
        for k in range(1, LINE):
            to = lax.rem(place[axis] + k, LINE)
            pl.semaphore_signal(
                barrier, inc=1, device_id=axis_target(axis, to), device_id_type=MESH
            )

    tokens = cot_ref.shape[1]
    for q in range(4):
        row = lax.broadcasted_iota(jnp.int32, (1024, 256), 0)
        col = lax.broadcasted_iota(jnp.int32, (1024, 256), 1)
        j = row % 4
        qq = (row // 4) % 4
        zh = (row // 16) % 2
        y = (row // 32) % 4
        x = (row // 128) % 4
        c = row // 512
        source = (((zh * 4 + x) * 4 + y) * 2 + c) * 4 + j
        pick = jnp.where((source == col) & (qq == q), 1.0, 0.0).astype(jnp.bfloat16)
        rows_ref[:, q * tokens : (q + 1) * tokens] = lax.dot_general(
            pick,
            cot_ref[...],
            (((1,), (0,)), ((), ())),
            preferred_element_type=jnp.float32,
        ).astype(jnp.bfloat16)
        for m in range(2):
            wide_ref[q * tokens : (q + 1) * tokens, m * 512 : (m + 1) * 512] = text_ref[
                :, m * 2048 + q * 512 : m * 2048 + (q + 1) * 512
            ]

    def block(i, carry):
        rows = rows_ref[pl.ds(pl.multiple_of(i * 128, 128), 128), :]
        for m in range(2):
            value = jnp.dot(
                rows, wide_ref[:, m * 512 : (m + 1) * 512], preferred_element_type=jnp.float32
            ).astype(jnp.bfloat16)
            value = value.reshape(4, 2, 16, 512)
            at = lax.rem(i, 4)
            for zh in range(2):
                own_a[i // 4, at, :, zh * 2 + m] = value[:, zh, :, :256]
                own_b[i // 4, at, :, zh * 2 + m] = value[:, zh, :, 256:]
        return carry

    lax.fori_loop(0, 8, block, 0)

    pl.semaphore_wait(barrier, 10)

    firsts = (own_a, own_b, conv_ref)
    copies = []
    for c in range(3):
        copy = pltpu.make_async_remote_copy(
            src_ref=firsts[c].at[other],
            dst_ref=core_in.at[c],
            send_sem=send_sems.at[c],
            recv_sem=recv_sems.at[c],
            device_id=axis_target("core", other),
            device_id_type=MESH,
        )
        copy.start()
        copies.append(copy)

    def exchange(c, stage, source, left, into):
        axis = ORDERS[c][stage]
        started = []
        for k in range(1, LINE):
            to = lax.rem(place[axis] + k, LINE)
            slot = 3 + (c * 3 + stage) * 3 + k - 1
            copy = pltpu.make_async_remote_copy(
                src_ref=part_of(source.at[c], left, axis, to),
                dst_ref=into.at[c, k - 1],
                send_sem=send_sems.at[slot],
                recv_sem=recv_sems.at[slot],
                device_id=axis_target(axis, to),
                device_id_type=MESH,
            )
            copy.start()
            started.append(copy)
        return started

    lines = []
    for c in range(3):
        copies[c].wait_recv()

        def add(i, carry, c=c):
            held[c, i] = (
                firsts[c][core, i].astype(jnp.float32) + core_in[c, i].astype(jnp.float32)
            ).astype(jnp.bfloat16)
            return carry

        lax.fori_loop(0, LINE, add, 0)
        lines.append(exchange(c, 0, held, ("x", "y", "z"), line_in))

    def own_part(ref, c, left, axis):
        index = tuple(place[axis] if name == axis else slice(None) for name in left)
        return ref[(c,) + index]

    seconds = []
    for c in range(3):
        axis = ORDERS[c][0]
        for copy in lines[c]:
            copy.wait_recv()
        for i in range(LINE):
            rest = [name for name in ("x", "y", "z") if name != axis]
            index = tuple(
                place[axis] if name == axis else (i if name == rest[0] else slice(None))
                for name in ("x", "y", "z")
            )
            value = held[(c,) + index].astype(jnp.float32)
            for k in range(LINE - 1):
                value = value + line_in[c, k, i].astype(jnp.float32)
            second[c, i] = value.astype(jnp.bfloat16)
        left = tuple(name for name in ("x", "y", "z") if name != axis)
        seconds.append(exchange(c, 1, second, left, second_in))

    thirds = []
    for c in range(3):
        left = tuple(name for name in ("x", "y", "z") if name != ORDERS[c][0])
        axis = ORDERS[c][1]
        for copy in seconds[c]:
            copy.wait_recv()
        value = own_part(second, c, left, axis).astype(jnp.float32)
        for k in range(LINE - 1):
            value = value + second_in[c, k].astype(jnp.float32)
        third[c] = value.astype(jnp.bfloat16)
        thirds.append(exchange(c, 2, third, (ORDERS[c][2],), third_in))

    for c in range(3):
        axis = ORDERS[c][2]
        for copy in thirds[c]:
            copy.wait_recv()
        value = third[c, place[axis]].astype(jnp.float32)
        for k in range(LINE - 1):
            value = value + third_in[c, k].astype(jnp.float32)
        total_ref[:, c * 256 : (c + 1) * 256] = value

    value = total_ref[...]
    square = value * value
    kv_line = jnp.sum(square[:, :512], axis=0, keepdims=True)
    kv_line = (
        kv_line[:, :128] + kv_line[:, 128:256] + kv_line[:, 256:384] + kv_line[:, 384:512]
    )
    conv_line = jnp.sum(square[:, 512:], axis=0, keepdims=True)
    row = lax.broadcasted_iota(jnp.int32, (8, 128), 0)
    tile = jnp.where(row == 0, kv_line, 0.0)
    tile = jnp.where(row == 1, conv_line[:, :128], tile)
    tile = jnp.where(row == 2, conv_line[:, 128:], tile)
    tile = jnp.where(row == 3, loss_ref[...], tile)
    at = 0
    for stage, axis in enumerate(("core", "x", "y", "z")):
        size = 2 if axis == "core" else LINE
        slots[stage, place[axis]] = tile
        started = []
        for k in range(1, size):
            to = lax.rem(place[axis] + k, size)
            copy = pltpu.make_async_remote_copy(
                src_ref=slots.at[stage, place[axis]],
                dst_ref=slots.at[stage, place[axis]],
                send_sem=slot_send.at[at],
                recv_sem=slot_recv.at[at],
                device_id=axis_target(axis, to),
                device_id_type=MESH,
            )
            copy.start()
            started.append(copy)
            at += 1
        for copy in started:
            copy.wait_recv()
        tile = slots[stage, 0]
        for k in range(1, size):
            tile = tile + slots[stage, k]
        for copy in started:
            copy.wait_send()
    sums = jnp.sum(tile, axis=1, keepdims=True)
    kv_scale = lax.rsqrt(sums[0:1] / counts[0] + 1e-06)
    one_scale = lax.rsqrt(sums[1:2] / counts[1] + 1e-06)
    two_scale = lax.rsqrt(sums[2:3] / counts[1] + 1e-06)
    one_ref[...] = total_ref[0:9, 512:640] * one_scale
    two_ref[...] = total_ref[0:9, 640:768] * two_scale
    for q in range(4):
        kv_ref[:, q * 512 : (q + 1) * 512] = total_ref[q * 4 : (q + 1) * 4, 0:512] * kv_scale
    mean_ref[...] = jnp.broadcast_to(sums[3:4] / counts[2], mean_ref.shape)
    for copy in copies:
        copy.wait_send()
    for group in lines + seconds + thirds:
        for copy in group:
            copy.wait_send()


def finish(text, cot, conv, loss, counts):
    bf16, f32 = jnp.bfloat16, jnp.float32
    return pl.pallas_call(
        functools.partial(finish_kernel, counts),
        out_shape=(
            jax.ShapeDtypeStruct((9, 128), f32),
            jax.ShapeDtypeStruct((9, 128), f32),
            jax.ShapeDtypeStruct((4, 2048), f32),
            jax.ShapeDtypeStruct((1, 128), f32),
        ),
        in_specs=[pl.BlockSpec(memory_space=pltpu.VMEM)] * 4,
        out_specs=[pl.BlockSpec(memory_space=pltpu.VMEM)] * 4,
        scratch_shapes=[
            pltpu.VMEM((1024, 1024), bf16),
            pltpu.VMEM((1024, 1024), bf16),
            pltpu.VMEM((2, 4, 4, 4, 16, 256), bf16),
            pltpu.VMEM((2, 4, 4, 4, 16, 256), bf16),
            pltpu.VMEM((3, 4, 4, 4, 16, 256), bf16),
            pltpu.VMEM((3, 4, 4, 4, 16, 256), bf16),
            pltpu.VMEM((3, 3, 4, 4, 16, 256), bf16),
            pltpu.VMEM((3, 4, 4, 16, 256), bf16),
            pltpu.VMEM((3, 3, 4, 16, 256), bf16),
            pltpu.VMEM((3, 4, 16, 256), bf16),
            pltpu.VMEM((3, 3, 16, 256), bf16),
            pltpu.VMEM((16, 768), f32),
            pltpu.VMEM((4, 4, 8, 128), f32),
            pltpu.SemaphoreType.DMA((30,)),
            pltpu.SemaphoreType.DMA((30,)),
            pltpu.SemaphoreType.DMA((10,)),
            pltpu.SemaphoreType.DMA((10,)),
        ],
        compiler_params=pltpu.CompilerParams(
            collective_id=0, has_side_effects=True, vmem_limit_bytes=16 * 2**20
        ),
        cost_estimate=pl.CostEstimate(
            flops=3 * 10**9, bytes_accessed=8 * 10**6, transcendentals=0
        ),
        name="finish",
    )(text, cot, conv, loss)


def local(
    clean,
    noise,
    lowres,
    aug_noise,
    timesteps,
    aug_levels,
    lengths,
    text,
    w_stem,
    w_time,
    conv_one,
    conv_two,
    kv_weight,
    w_query,
    w_output,
    w_head,
):
    images = clean.shape[0]
    tokens = text.shape[1]
    features = text.shape[2]
    width = kv_weight.shape[1]
    half = kv_weight.shape[0]
    bf16, f32 = jnp.bfloat16, jnp.float32
    far = lax.ppermute(kv_weight, "mp", [(0, 1), (1, 0)])

    step, level = timesteps[:, None], aug_levels[:, None]
    which = np.arange(4)
    signal = signal_level(jnp.where(which < 2, step, level))
    coefs = jnp.sqrt(jnp.where(which % 2 == 0, signal, 1.0 - signal))
    lane = np.arange(4 * FREQS)
    freqs = jnp.exp(-math.log(10000.0) * (lane % FREQS).astype(np.float32) / FREQS)
    angles = jnp.where(lane < 2 * FREQS, step, level).astype(f32) * freqs
    feature = jnp.where(lane % (2 * FREQS) < FREQS, jnp.sin(angles), jnp.cos(angles))
    clean, noise, lowres, aug_noise = (
        jnp.transpose(a, (1, 0, 2)) for a in (clean, noise, lowres, aug_noise)
    )
    made = forward(
        coefs, clean, noise, lowres, aug_noise, w_stem, feature, w_time, conv_one, conv_two
    )
    mp = lax.axis_index("mp").astype(jnp.int32).reshape(1)
    flat_text = text.reshape(images * tokens, features)
    cot, conv, loss = backward(
        mp, lengths, noise, flat_text, kv_weight, far, made, conv_two, w_query, w_output, w_head
    )
    counts = (
        2 * half * width,
        conv_one.shape[0] * conv_one.shape[1],
        images * lax.axis_size(DP_MP) * clean.shape[0] * clean.shape[2],
    )
    conv_one_update, conv_two_update, kv, mean = finish(flat_text, cot, conv, loss, counts)
    return (conv_one_update, conv_two_update, kv.T, mean[0, 0])


def solution(mesh):
    finer = Mesh(
        mesh.devices.reshape(2, 4, 4, 2, mesh.shape["mp"]), ("dp_0", "dp_1", "dp_2", "dp_3", "mp")
    )
    placed = (
        P(DP_MP, None, None),
        P(DP_MP, None, None),
        P(DP_MP, None, None),
        P(DP_MP, None, None),
        P(DP_MP),
        P(DP_MP),
        P(DP_MP),
        P(DP_MP, None, None),
        P(),
        P(),
        P(),
        P(),
        P("mp", None),
        P(),
        P(),
        P(),
    )
    return jax.shard_map(
        local,
        mesh=finer,
        in_specs=placed,
        out_specs=(P(DP_MP, None), P(DP_MP, None), P("mp", DP), P()),
        check_vma=False,
    )
```

```python
import functools
import math

import jax
import jax.numpy as jnp
import numpy as np
from jax import lax
from jax.sharding import Mesh
from jax.sharding import PartitionSpec as P
from jax.experimental import pallas as pl
from jax.experimental.pallas import tpu as pltpu

S = 64
GROUPS = 32
HEADS = 2
HEAD_DIM = 64
FREQS = 64
STEPS = 1000
DP_MP = ("dp_0", "dp_1", "dp_2", "dp_3", "mp")
DP = ("dp_0", "dp_1", "dp_2", "dp_3")


def signal_level(index):
    ratio = (index.astype(jnp.float32) / STEPS + 0.008) / 1.008
    cosine = jnp.cos(ratio * (math.pi / 2.0))
    return cosine * cosine


PIXELS = S * S
CHUNK = 512
CHUNKS = PIXELS // CHUNK
EDGE = S
C = 128


def group_total(line):
    lane = lax.broadcasted_iota(jnp.int32, line.shape, 1)
    pair = line + jnp.where(
        lane % 2 == 0, pltpu.roll(line, C - 1, 1), pltpu.roll(line, 1, 1)
    )
    return pair + jnp.where(
        lane % 4 < 2, pltpu.roll(pair, C - 2, 1), pltpu.roll(pair, 2, 1)
    )


def group_mean(total):
    line = jnp.broadcast_to(jnp.sum(total, axis=0, keepdims=True), (8, C)) / PIXELS
    return group_total(line)[0:1] / (C // GROUPS)


def row_of(value, i):
    row = value[0:1]
    for r in range(1, value.shape[0]):
        row = jnp.where(i == r, value[r : r + 1], row)
    return row


def fold(value):
    return jnp.sum(value.reshape(-1, 8, value.shape[-1]), axis=0)


def spread(act):
    column = lax.broadcasted_iota(jnp.int32, act.shape, 0) % S
    rows = act.shape[0]
    left = jnp.where(column == 0, 0.0, pltpu.roll(act, 1, 0))
    right = jnp.where(column == S - 1, 0.0, pltpu.roll(act, rows - 1, 0))
    return jnp.concatenate(
        [left.astype(jnp.bfloat16), act.astype(jnp.bfloat16), right.astype(jnp.bfloat16)], axis=1
    )


def span(j, size=CHUNK):
    return pl.ds(pl.multiple_of(j * size, size), size)


LINES = CHUNK // S


def inside(j, shift=1):
    return pl.ds(j * LINES + shift, LINES)


def clear_edges(ref, i):
    zero = jnp.zeros((S, ref.shape[-1]), jnp.bfloat16)
    ref[i, 0] = zero
    ref[i, S + 1] = zero


CONV = 2048
PAIRS = CONV // (2 * S)


def fill_pairs(pair_ref, block_of):
    for iy in range(4):
        for dx in range(3):
            at = (iy * 3 + dx) * C
            for oy in range(2):
                dy = iy - oy
                block = (
                    block_of(dy * 3 + dx) if 0 <= dy < 3 else jnp.zeros((C, C), jnp.bfloat16)
                )
                pair_ref[at : at + C, oy * C : (oy + 1) * C] = block


def conv_rows(wide_ref, i, j, pair_ref):
    rows = [
        jnp.concatenate([wide_ref[i, 2 * (j * PAIRS + t) + iy] for iy in range(4)], axis=1)
        for t in range(PAIRS)
    ]
    value = jnp.dot(
        jnp.concatenate(rows, axis=0), pair_ref[...], preferred_element_type=jnp.float32
    )
    lines = []
    for t in range(PAIRS):
        for oy in range(2):
            lines.append(value[t * S : (t + 1) * S, oy * C : (oy + 1) * C])
    return jnp.concatenate(lines, axis=0)


def loop_sum(body, size=CHUNK):
    return lax.fori_loop(0, PIXELS // size, body, jnp.zeros((8, C), jnp.float32))


def forward_kernel(
    coef_ref,
    feature_ref,
    clean_in,
    noise_in,
    low_in,
    aug_in,
    stem_in,
    time_in,
    one_in,
    two_in,
    mid_ref,
    out_ref,
    wide_one,
    wide_two,
    stats_ref,
    clean_ref,
    noise_ref,
    low_ref,
    aug_ref,
    stem_ref,
    time_ref,
    one_ref,
    two_ref,
    planes_ref,
    stems_ref,
    embed_ref,
    lhs_ref,
    pair_one,
    pair_two,
    sems,
):
    sources = (stem_in, time_in, clean_in, noise_in, low_in, aug_in, one_in, two_in)
    targets = (stem_ref, time_ref, clean_ref, noise_ref, low_ref, aug_ref, one_ref, two_ref)
    copies = [
        pltpu.make_async_copy(sources[n], targets[n], sems.at[n]) for n in range(len(sources))
    ]
    for copy in copies:
        copy.start()
    images = clean_ref.shape[1]
    for copy in copies:
        copy.wait()
    fill_pairs(pair_one, lambda tap: one_ref[tap * C : (tap + 1) * C])
    fill_pairs(pair_two, lambda tap: two_ref[tap * C : (tap + 1) * C])
    w = jnp.concatenate([stem_ref[...], jnp.zeros((2, C), jnp.float32)], axis=0)
    w1 = w.astype(jnp.bfloat16).astype(jnp.float32)
    w2 = (w - w1).astype(jnp.bfloat16).astype(jnp.float32)
    w3 = w - w1 - w2
    stems_ref[...] = jnp.concatenate([w1, w2, w1, w3, w2, w1], axis=0).astype(jnp.bfloat16)
    feature = jnp.concatenate(
        [feature_ref[...], jnp.zeros((8 - images, 2 * C), jnp.float32)], axis=0
    )
    embed = jnp.dot(
        feature,
        time_ref[...],
        precision=lax.Precision.HIGHEST,
        preferred_element_type=jnp.float32,
    )
    embed_ref[...] = embed * jax.nn.sigmoid(embed)
    planes_ref[...] = jnp.zeros(planes_ref.shape, jnp.float32)

    def image(i, carry):
        for k in range(3):
            planes_ref[k : k + 1] = (
                coef_ref[i, 0] * row_of(clean_ref[k], i)
                + coef_ref[i, 1] * row_of(noise_ref[k], i)
            )
            planes_ref[3 + k : 4 + k] = (
                coef_ref[i, 2] * row_of(low_ref[k], i) + coef_ref[i, 3] * row_of(aug_ref[k], i)
            )
        s = planes_ref[...]
        s1 = s.astype(jnp.bfloat16).astype(jnp.float32)
        s2 = (s - s1).astype(jnp.bfloat16).astype(jnp.float32)
        s3 = s - s1 - s2
        lhs_ref[...] = jnp.concatenate([s1, s1, s2, s1, s2, s3], axis=0).astype(jnp.bfloat16)
        clear_edges(wide_one, i)
        clear_edges(wide_two, i)

        def stem(j, total):
            h = lax.dot_general(
                lhs_ref[:, span(j)],
                stems_ref[...],
                (((0,), (0,)), ((), ())),
                preferred_element_type=jnp.float32,
            )
            mid_ref[i, span(j)] = h
            return total + fold(h)

        def variance(ref, mean):
            def body(j, total):
                centred = ref[i, span(j)] - mean
                return total + fold(centred * centred)

            return lax.rsqrt(group_mean(loop_sum(body)) + 1e-05)

        mean_one = group_mean(loop_sum(stem))
        inv_one = variance(mid_ref, mean_one)

        def first(j, carry):
            act = (mid_ref[i, span(j)] - mean_one) * inv_one
            wide_one[i, inside(j)] = spread(act * jax.nn.sigmoid(act)).reshape(LINES, S, 3 * C)
            return carry

        lax.fori_loop(0, CHUNKS, first, 0)

        def conv_first(j, total):
            value = conv_rows(wide_one, i, j, pair_one)
            out_ref[i, span(j, CONV)] = value
            return total + fold(value)

        mean_two = group_mean(loop_sum(conv_first, CONV))
        inv_two = variance(out_ref, mean_two)
        gain = 1.0 + row_of(embed_ref[0:images, 0:C], i)
        shift = row_of(embed_ref[0:images, C : 2 * C], i)

        def next_act(j, carry):
            act = (out_ref[i, span(j)] - mean_two) * inv_two * gain + shift
            wide_two[i, inside(j)] = spread(act * jax.nn.sigmoid(act)).reshape(LINES, S, 3 * C)
            return carry

        lax.fori_loop(0, CHUNKS, next_act, 0)

        def conv_second(j, total):
            value = mid_ref[i, span(j, CONV)] + conv_rows(wide_two, i, j, pair_two)
            mid_ref[i, span(j, CONV)] = value
            return total + fold(value)

        mean_three = group_mean(loop_sum(conv_second, CONV))
        inv_three = variance(mid_ref, mean_three)
        stats_ref[i] = jnp.concatenate(
            [mean_two, inv_two, mean_three, inv_three, gain, shift, gain, shift], axis=0
        )
        return carry

    lax.fori_loop(0, images, image, 0)


def forward(coefs, feature, *arrays):
    images = feature.shape[0]
    bf16, f32 = jnp.bfloat16, jnp.float32
    wide = jax.ShapeDtypeStruct((images, S + 2, S, 3 * C), bf16)
    flat = jax.ShapeDtypeStruct((images, PIXELS, C), f32)
    return pl.pallas_call(
        forward_kernel,
        out_shape=(flat, flat, wide, wide, jax.ShapeDtypeStruct((images, 8, C), f32)),
        in_specs=[
            pl.BlockSpec(memory_space=pltpu.SMEM),
            pl.BlockSpec(memory_space=pltpu.VMEM),
        ]
        + [pl.BlockSpec(memory_space=pltpu.HBM)] * 8,
        out_specs=[pl.BlockSpec(memory_space=pltpu.VMEM)] * 5,
        scratch_shapes=[pltpu.VMEM(a.shape, a.dtype) for a in arrays]
        + [
            pltpu.VMEM((8, PIXELS), f32),
            pltpu.VMEM((48, C), bf16),
            pltpu.VMEM((8, 2 * C), f32),
            pltpu.VMEM((48, PIXELS), bf16),
            pltpu.VMEM((12 * C, 2 * C), bf16),
            pltpu.VMEM((12 * C, 2 * C), bf16),
            pltpu.SemaphoreType.DMA((8,)),
        ],
        compiler_params=pltpu.CompilerParams(vmem_limit_bytes=LIMIT_F * 2**20),
        cost_estimate=pl.CostEstimate(
            flops=10**10, bytes_accessed=22 * 10**6, transcendentals=2 * 10**6
        ),
        name="forward",
    )(coefs, feature, *arrays)


TN = (((0,), (0,)), ((), ()))
NT = (((1,), (1,)), ((), ()))


def mm(a, b, dims=(((1,), (0,)), ((), ()))):
    return lax.dot_general(a, b, dims, preferred_element_type=jnp.float32)


def attend_kernel(
    half_ref,
    lengths_ref,
    noise_ref,
    text_ref,
    near_ref,
    far_ref,
    mid_ref,
    stats_ref,
    query_ref,
    output_ref,
    heads_ref,
    cot_ref,
    wide_grad,
    loss_ref,
    kv_ref,
    key_ref,
    val_ref,
    dkey_ref,
    dval_ref,
    dnorm_ref,
    dout_ref,
    head_ref,
    goal_ref,
):
    bf16, f32 = jnp.bfloat16, jnp.float32
    images = noise_ref.shape[1]
    tokens = text_ref.shape[0] // images
    half = near_ref.shape[0]
    mp = half_ref[0]
    here = pl.ds(pl.multiple_of(mp * half, half), half)
    there = pl.ds(pl.multiple_of((1 - mp) * half, half), half)
    kv_ref[...] = (
        mm(text_ref[:, here], near_ref[...]) + mm(text_ref[:, there], far_ref[...])
    ).astype(bf16)
    head_ref[...] = jnp.concatenate(
        [heads_ref[...].astype(f32), jnp.zeros((8 - heads_ref.shape[0], C), f32)], axis=0
    ).astype(bf16)
    goal_ref[...] = jnp.zeros(goal_ref.shape, f32)
    lane = lax.broadcasted_iota(jnp.int32, (tokens, C), 1)
    nothing = jnp.zeros((8, C), f32)

    def image(i, loss):
        clear_edges(wide_grad, i)
        for k in range(3):
            goal_ref[k : k + 1] = row_of(noise_ref[k], i)
        both = kv_ref[pl.ds(pl.multiple_of(i * tokens, tokens), tokens), :]
        zero = jnp.zeros((tokens, C), bf16)
        low = lane < HEAD_DIM
        key_ref[...] = jnp.concatenate(
            [jnp.where(low, both[:, :C], zero), jnp.where(low, zero, both[:, :C])], axis=0
        )
        val_ref[...] = jnp.concatenate(
            [jnp.where(low, both[:, C:], zero), jnp.where(low, zero, both[:, C:])], axis=0
        )
        dkey_ref[...] = jnp.zeros(dkey_ref.shape, f32)
        dval_ref[...] = jnp.zeros(dval_ref.shape, f32)
        mean_three, inv_three = stats_ref[i, 2:3], stats_ref[i, 3:4]
        keep = lax.broadcasted_iota(jnp.int32, (ATTEND, tokens), 1) < lengths_ref[i]

        def attend(j, carry):
            total, moment, loss = carry
            mid = mid_ref[i, span(j, ATTEND)]
            hat = (mid - mean_three) * inv_three
            query = (mm(hat.astype(bf16), query_ref[...]) * HEAD_DIM ** (-0.5)).astype(bf16)
            scores = mm(query, key_ref[...], NT)
            probs = []
            for h in range(HEADS):
                one = jnp.where(keep, scores[:, h * tokens : (h + 1) * tokens], -1e30)
                one = jnp.exp(one - jnp.max(one, axis=1, keepdims=True))
                probs.append(one / jnp.sum(one, axis=1, keepdims=True))
            rounded = jnp.concatenate([p.astype(bf16) for p in probs], axis=1)
            attended = mm(rounded, val_ref[...]).astype(bf16)
            out = (mid + mm(attended, output_ref[...])).astype(bf16)
            pred = mm(out, head_ref[...], NT)
            error = pred - goal_ref[:, span(j, ATTEND)].T
            loss = loss + fold(error * error)
            dout = mm((2.0 * error).astype(bf16), head_ref[...]).astype(bf16)
            dout_ref[span(j, ATTEND)] = dout
            datt = mm(dout, output_ref[...], NT).astype(bf16)
            dprobs = mm(datt, val_ref[...], NT).astype(bf16).astype(f32)
            dval_ref[...] += mm(datt, rounded, TN)
            dscores = []
            for h in range(HEADS):
                one = dprobs[:, h * tokens : (h + 1) * tokens]
                inner = jnp.sum(one * probs[h], axis=1, keepdims=True)
                dscores.append((probs[h] * (one - inner)).astype(bf16))
            dscores = jnp.concatenate(dscores, axis=1)
            dkey_ref[...] += mm(query, dscores, TN)
            dquery = mm(dscores, key_ref[...]).astype(bf16)
            dnorm = (mm(dquery, query_ref[...], NT) * HEAD_DIM ** (-0.5)).astype(bf16)
            dnorm_ref[span(j, ATTEND)] = dnorm
            dnorm = dnorm.astype(f32)
            return (total + fold(dnorm), moment + fold(dnorm * hat), loss)

        total, moment, loss = lax.fori_loop(0, PIXELS // ATTEND, attend, (nothing, nothing, loss))
        low_row = lax.broadcasted_iota(jnp.int32, (C, tokens), 0) < HEAD_DIM
        cots = [
            jnp.where(low_row, ref[:, :tokens], ref[:, tokens:]) for ref in (dkey_ref, dval_ref)
        ]
        cot_ref[:, pl.ds(pl.multiple_of(i * tokens, tokens), tokens)] = jnp.concatenate(
            cots, axis=0
        ).astype(bf16)
        first, second = group_mean(total), group_mean(moment)

        def middle(j, carry):
            hat = (mid_ref[i, span(j)] - mean_three) * inv_three
            grad = dout_ref[span(j)].astype(f32) + inv_three * (
                dnorm_ref[span(j)].astype(f32) - first - hat * second
            )
            wide_grad[i, inside(j)] = spread(grad).reshape(LINES, S, 3 * C)
            return carry

        lax.fori_loop(0, CHUNKS, middle, 0)

        return loss

    loss = lax.fori_loop(0, images, image, jnp.zeros((8, 8), f32))
    loss_ref[...] = jnp.broadcast_to(
        jnp.sum(jnp.sum(loss, axis=0, keepdims=True), axis=1, keepdims=True) / C, (1, C)
    )


def attention(half, lengths, noise, text, near, far, mid, stats, w_query, w_output, head):
    images = noise.shape[1]
    bf16, f32 = jnp.bfloat16, jnp.float32
    tokens = text.shape[0] // images
    vmem = pl.BlockSpec(memory_space=pltpu.VMEM)
    smem = pl.BlockSpec(memory_space=pltpu.SMEM)
    return pl.pallas_call(
        attend_kernel,
        out_shape=(
            jax.ShapeDtypeStruct((2 * C, images * tokens), bf16),
            jax.ShapeDtypeStruct((images, S + 2, S, 3 * C), bf16),
            jax.ShapeDtypeStruct((1, C), f32),
        ),
        in_specs=[smem] * 2 + [vmem] * 9,
        out_specs=[vmem] * 3,
        scratch_shapes=[
            pltpu.VMEM((images * tokens, 2 * C), bf16),
            pltpu.VMEM((2 * tokens, C), bf16),
            pltpu.VMEM((2 * tokens, C), bf16),
            pltpu.VMEM((C, 2 * tokens), f32),
            pltpu.VMEM((C, 2 * tokens), f32),
            pltpu.VMEM((PIXELS, C), bf16),
            pltpu.VMEM((PIXELS, C), bf16),
            pltpu.VMEM((8, C), bf16),
            pltpu.VMEM((8, PIXELS), f32),
        ],
        compiler_params=pltpu.CompilerParams(vmem_limit_bytes=LIMIT_A * 2**20),
        cost_estimate=pl.CostEstimate(
            flops=10**10, bytes_accessed=16 * 10**6, transcendentals=6 * 10**6
        ),
        name="attention",
    )(half, lengths, noise, text, near, far, mid, stats, w_query, w_output, head)


ATTEND = 1024
LIMIT_F = 12
LIMIT_A = 16
LIMIT_T = 20


MESH = pl.DeviceIdType.MESH
LINE = 4
WIDTHS = (256, 256, 128, 128)
ORDERS = (("x", "y", "z"), ("y", "z", "x"), ("z", "x", "y"), ("z", "x", "y"))
COLUMNS = (0, 256, 640, 512)


def axis_target(axis, to):
    if axis == "x":
        return {"dp_1": to}
    if axis == "y":
        return {"dp_2": to}
    if axis == "z":
        return {"dp_0": to // 2, "mp": lax.rem(to, 2)}
    return {"dp_3": to}


def remote(source, target, send, recv, axis, to):
    copy = pltpu.make_async_remote_copy(
        src_ref=source,
        dst_ref=target,
        send_sem=send,
        recv_sem=recv,
        device_id=axis_target(axis, to),
        device_id_type=MESH,
    )
    copy.start()
    return copy


def finish_kernel(
    counts,
    text_ref,
    cot_ref,
    loss_ref,
    out_ref,
    wide_one,
    wide_two,
    wide_grad,
    stats_ref,
    two_ref,
    one_out,
    two_out,
    kv_out,
    mean_out,
    rows_ref,
    dhat_ref,
    grad_ref,
    flat_ref,
    sum_ref,
    flip_ref,
    grad_pad,
    total_ref,
    slots,
    send_sems,
    recv_sems,
    slot_send,
    slot_recv,
    *stages,
):
    bf16, f32 = jnp.bfloat16, jnp.float32
    images = stats_ref.shape[0]
    own, core_in, held, line_in, second, second_in, third, third_in = (
        stages[n * 4 : (n + 1) * 4] for n in range(8)
    )
    place = {
        "x": lax.axis_index("dp_1"),
        "y": lax.axis_index("dp_2"),
        "z": lax.axis_index("dp_0") * 2 + lax.axis_index("mp"),
        "core": lax.axis_index("dp_3"),
    }
    core = place["core"]
    other = 1 - core
    barrier = pltpu.get_barrier_semaphore()
    for outer, inner, size in (("z", "core", 2), ("x", "y", LINE)):
        for k in range(1, LINE * size):
            to = {
                **axis_target(outer, lax.rem(place[outer] + k // size, LINE)),
                **axis_target(inner, lax.rem(place[inner] + k % size, size)),
            }
            pl.semaphore_signal(barrier, inc=1, device_id=to, device_id_type=MESH)

    sent = []

    def start_core(c):
        copy = remote(
            own[c].at[other],
            core_in[c],
            send_sems.at[c * 10],
            recv_sems.at[c * 10],
            "core",
            other,
        )
        sent.append(copy)
        return [copy]

    def part_of(left, axis, at):
        return tuple(at if name == axis else slice(None) for name in left)

    def exchange(c, stage, source, left, into):
        axis = ORDERS[c][stage]
        started = []
        for k in range(1, LINE):
            to = lax.rem(place[axis] + k, LINE)
            slot = c * 10 + stage * 3 + k
            started.append(
                remote(
                    source[c].at[part_of(left, axis, to)],
                    into[c].at[k - 1],
                    send_sems.at[slot],
                    recv_sems.at[slot],
                    axis,
                    to,
                )
            )
        sent.extend(started)
        return started

    def arrive(copies):
        for copy in copies:
            copy.wait_recv()

    def to_first(c, copies):
        arrive(copies)

        def add(i, carry):
            held[c][i] = (own[c][core, i].astype(f32) + core_in[c][i].astype(f32)).astype(bf16)
            return carry

        lax.fori_loop(0, LINE, add, 0)
        return exchange(c, 0, held, ("x", "y", "z"), line_in)

    def to_second(c, copies):
        arrive(copies)
        axis = ORDERS[c][0]
        rest = [name for name in ("x", "y", "z") if name != axis]
        for i in range(LINE):
            index = tuple(
                place[axis] if name == axis else (i if name == rest[0] else slice(None))
                for name in ("x", "y", "z")
            )
            value = held[c][index].astype(f32)
            for k in range(LINE - 1):
                value = value + line_in[c][k, i].astype(f32)
            second[c][i] = value.astype(bf16)
        return exchange(c, 1, second, tuple(rest), second_in)

    def to_third(c, copies):
        arrive(copies)
        left = tuple(name for name in ("x", "y", "z") if name != ORDERS[c][0])
        axis = ORDERS[c][1]
        value = second[c][part_of(left, axis, place[axis])].astype(f32)
        for k in range(LINE - 1):
            value = value + second_in[c][k].astype(f32)
        third[c][...] = value.astype(bf16)
        return exchange(c, 2, third, (ORDERS[c][2],), third_in)

    def to_total(c, copies):
        arrive(copies)
        value = third[c][place[ORDERS[c][2]]].astype(f32)
        for k in range(LINE - 1):
            value = value + third_in[c][k].astype(f32)
        total_ref[:, COLUMNS[c] : COLUMNS[c] + WIDTHS[c]] = value

    tokens = cot_ref.shape[1]
    row = lax.broadcasted_iota(jnp.int32, (1024, 256), 0)
    col = lax.broadcasted_iota(jnp.int32, (1024, 256), 1)
    owner = ((row // 16) % 2 * 32 + row // 32 % 16 * 2 + row // 512) * 4 + row % 4
    pick = jnp.where(owner == col, 1.0, 0.0).astype(bf16)
    picked = mm(pick, cot_ref[...])
    quarter = (row // 4) % 4
    for q in range(4):
        rows_ref[:, q * tokens : (q + 1) * tokens] = jnp.where(
            quarter[:, :tokens] == q, picked, 0.0
        ).astype(bf16)

    def block(m, carry):
        for c in range(2):
            at = m * 2048 + c * 256
            wide = jnp.concatenate(
                [
                    text_ref[:, pl.ds(pl.multiple_of(at + q * 512, 256), 256)]
                    for q in range(4)
                ],
                axis=0,
            )
            for half in range(2):
                value = mm(rows_ref[half * 512 : (half + 1) * 512, :], wide).astype(bf16)
                value = value.reshape(4, 4, 2, 16, 256)
                for zh in range(2):
                    own[c][half, :, :, zh * 2 + m] = value[:, :, zh]
        return carry

    lax.fori_loop(0, 2, block, 0)
    pl.semaphore_wait(barrier, 22)
    first_kv = [start_core(0), start_core(1)]

    fill_pairs(flip_ref, lambda tap: two_ref[(8 - tap) * C : (9 - tap) * C].T)
    clear_edges(grad_pad, 0)
    sum_ref[...] = jnp.zeros(sum_ref.shape, f32)
    flat_ref[:, 9 * C :] = jnp.zeros((2, 16, C), f32)
    nothing = jnp.zeros((8, C), f32)

    def weights(which, i, source, grad_of):
        grad_ref[...] = jnp.zeros(grad_ref.shape, f32)

        def body(j, carry):
            grads = [grad_of(inside(j, 2 - dy)).reshape(CHUNK, C) for dy in range(3)]
            grad_ref[...] += mm(
                jnp.concatenate(grads, axis=1), source[i, inside(j)].reshape(CHUNK, 3 * C), TN
            )
            return carry

        lax.fori_loop(0, CHUNKS, body, 0)
        sum_ref[which] += grad_ref[...].astype(bf16).astype(f32)

    def pack(which, c):
        for dy in range(3):
            for dx in range(3):
                at = (dy * 3 + dx) * C
                flat_ref[which, at : at + C] = sum_ref[
                    which, dy * C : (dy + 1) * C, dx * C : (dx + 1) * C
                ].T
        row = lax.broadcasted_iota(jnp.int32, (16, C), 0)

        for d in range(128):
            piece = jnp.where(row < 9, flat_ref[which, d * 9 : d * 9 + 16], 0.0).astype(bf16)
            own[c][d // 2 % 2, d // 16 % 4, d // 4 % 4, d // 64 * 2 + d % 2] = piece

    def act_grad(i):
        mean_two, inv_two = stats_ref[i, 0:1], stats_ref[i, 1:2]
        gain, shift = stats_ref[i, 4:5], stats_ref[i, 5:6]

        def inner(j, carry):
            total, moment = carry
            dact = conv_rows(wide_grad, i, j, flip_ref).astype(bf16).astype(f32)
            at = span(j, CONV)
            hat = (out_ref[i, at] - mean_two) * inv_two
            act = hat * gain + shift
            gate = jax.nn.sigmoid(act)
            dhat = dact * (gate * (1.0 + act * (1.0 - gate))) * gain
            dhat_ref[at] = dhat
            return (total + fold(dhat), moment + fold(dhat * hat))

        total, moment = lax.fori_loop(0, PIXELS // CONV, inner, (nothing, nothing))
        return mean_two, inv_two, group_mean(total), group_mean(moment)

    def early_grad(i, lines):
        mean_two, inv_two, first, moment = lines

        def early(j, carry):
            hat = (out_ref[i, span(j)] - mean_two) * inv_two
            grad = inv_two * (dhat_ref[span(j)] - first - hat * moment)
            grad_pad[0, inside(j)] = grad.astype(bf16).reshape(LINES, S, C)
            return carry

        lax.fori_loop(0, CHUNKS, early, 0)
        weights(0, i, wide_one, lambda at: grad_pad[0, at])

    for i in range(images):
        weights(1, i, wide_two, lambda at, i=i: wide_grad[i, at, :, C : 2 * C])
    copies = [to_first(0, first_kv[0]), to_first(1, first_kv[1])]
    pack(1, 2)
    copies.append(start_core(2))
    lines = act_grad(0)
    copies[2] = to_first(2, copies[2])
    early_grad(0, lines)
    for c in range(2):
        copies[c] = to_second(c, copies[c])
    lines = act_grad(1)
    copies[2] = to_second(2, copies[2])
    for c in range(2):
        copies[c] = to_third(c, copies[c])
    early_grad(1, lines)
    pack(0, 3)
    copies.append(start_core(3))
    copies[2] = to_third(2, copies[2])
    for c in range(2):
        to_total(c, copies[c])
    copies[3] = to_first(3, copies[3])
    to_total(2, copies[2])
    copies[3] = to_second(3, copies[3])
    copies[3] = to_third(3, copies[3])
    to_total(3, copies[3])

    value = total_ref[...]
    square = value * value
    kv_line = jnp.sum(square[:, :512], axis=0, keepdims=True)
    kv_line = (
        kv_line[:, :128] + kv_line[:, 128:256] + kv_line[:, 256:384] + kv_line[:, 384:512]
    )
    conv_line = jnp.sum(square[:, 512:], axis=0, keepdims=True)
    row = lax.broadcasted_iota(jnp.int32, (8, 128), 0)
    tile = jnp.where(row == 0, kv_line, 0.0)
    tile = jnp.where(row == 1, conv_line[:, :128], tile)
    tile = jnp.where(row == 2, conv_line[:, 128:], tile)
    tile = jnp.where(row == 3, loss_ref[...], tile)
    at = 0
    for stage, (outer, inner) in enumerate((("z", "core"), ("x", "y"))):
        sizes = (LINE, 2 if inner == "core" else LINE)
        mine = place[outer] * sizes[1] + place[inner]
        slots[stage, mine] = tile
        started = []
        for k in range(1, sizes[0] * sizes[1]):
            to = {
                **axis_target(outer, lax.rem(place[outer] + k // sizes[1], LINE)),
                **axis_target(inner, lax.rem(place[inner] + k % sizes[1], sizes[1])),
            }
            copy = pltpu.make_async_remote_copy(
                src_ref=slots.at[stage, mine],
                dst_ref=slots.at[stage, mine],
                send_sem=slot_send.at[at],
                recv_sem=slot_recv.at[at],
                device_id=to,
                device_id_type=MESH,
            )
            copy.start()
            started.append(copy)
            at += 1
        arrive(started)
        sent.extend(started)
        tile = slots[stage, 0]
        for k in range(1, sizes[0] * sizes[1]):
            tile = tile + slots[stage, k]
    sums = jnp.sum(tile, axis=1, keepdims=True)
    kv_scale = lax.rsqrt(sums[0:1] / counts[0] + 1e-06)
    one_scale = lax.rsqrt(sums[1:2] / counts[1] + 1e-06)
    two_scale = lax.rsqrt(sums[2:3] / counts[1] + 1e-06)
    one_out[...] = total_ref[0:9, 512:640] * one_scale
    two_out[...] = total_ref[0:9, 640:768] * two_scale
    for q in range(4):
        kv_out[:, q * 512 : (q + 1) * 512] = total_ref[q * 4 : (q + 1) * 4, 0:512] * kv_scale
    mean_out[...] = jnp.broadcast_to(sums[3:4] / counts[2], mean_out.shape)
    for copy in sent:
        copy.wait_send()


def finish(counts, *arrays):
    bf16, f32 = jnp.bfloat16, jnp.float32
    vmem = pl.BlockSpec(memory_space=pltpu.VMEM)
    stages = [
        (2, 4, 4, 4, 16),
        (4, 4, 4, 16),
        (4, 4, 4, 16),
        (3, 4, 4, 16),
        (4, 4, 16),
        (3, 4, 16),
        (4, 16),
        (3, 16),
    ]
    return pl.pallas_call(
        functools.partial(finish_kernel, counts),
        out_shape=(
            jax.ShapeDtypeStruct((9, 128), f32),
            jax.ShapeDtypeStruct((9, 128), f32),
            jax.ShapeDtypeStruct((4, 2048), f32),
            jax.ShapeDtypeStruct((1, 128), f32),
        ),
        in_specs=[vmem] * len(arrays),
        out_specs=[vmem] * 4,
        scratch_shapes=[
            pltpu.VMEM((1024, 1024), bf16),
            pltpu.VMEM((PIXELS, C), f32),
            pltpu.VMEM((3 * C, 3 * C), f32),
            pltpu.VMEM((2, 9 * C + 16, C), f32),
            pltpu.VMEM((2, 3 * C, 3 * C), f32),
            pltpu.VMEM((12 * C, 2 * C), bf16),
            pltpu.VMEM((1, S + 2, S, C), bf16),
            pltpu.VMEM((16, 768), f32),
            pltpu.VMEM((2, 16, 8, 128), f32),
            pltpu.SemaphoreType.DMA((40,)),
            pltpu.SemaphoreType.DMA((40,)),
            pltpu.SemaphoreType.DMA((22,)),
            pltpu.SemaphoreType.DMA((22,)),
        ]
        + [pltpu.VMEM((*shape, width), bf16) for shape in stages for width in WIDTHS],
        compiler_params=pltpu.CompilerParams(
            collective_id=0, has_side_effects=True, vmem_limit_bytes=LIMIT_T * 2**20
        ),
        cost_estimate=pl.CostEstimate(
            flops=2 * 10**10, bytes_accessed=30 * 10**6, transcendentals=2 * 10**6
        ),
        name="finish",
    )(*arrays)


def local(
    clean,
    noise,
    lowres,
    aug_noise,
    timesteps,
    aug_levels,
    lengths,
    text,
    w_stem,
    w_time,
    conv_one,
    conv_two,
    kv_weight,
    w_query,
    w_output,
    w_head,
):
    images = clean.shape[0]
    tokens = text.shape[1]
    features = text.shape[2]
    width = kv_weight.shape[1]
    half = kv_weight.shape[0]
    bf16, f32 = jnp.bfloat16, jnp.float32
    far = lax.ppermute(kv_weight, "mp", [(0, 1), (1, 0)])

    step, level = timesteps[:, None], aug_levels[:, None]
    which = np.arange(4)
    signal = signal_level(jnp.where(which < 2, step, level))
    coefs = jnp.sqrt(jnp.where(which % 2 == 0, signal, 1.0 - signal))
    lane = np.arange(4 * FREQS)
    freqs = jnp.exp(-math.log(10000.0) * (lane % FREQS).astype(np.float32) / FREQS)
    angles = jnp.where(lane < 2 * FREQS, step, level).astype(f32) * freqs
    feature = jnp.where(lane % (2 * FREQS) < FREQS, jnp.sin(angles), jnp.cos(angles))
    clean, noise, lowres, aug_noise = (
        jnp.transpose(a, (1, 0, 2)) for a in (clean, noise, lowres, aug_noise)
    )
    made = forward(
        coefs, feature, clean, noise, lowres, aug_noise, w_stem, w_time, conv_one, conv_two
    )
    mp = lax.axis_index("mp").astype(jnp.int32).reshape(1)
    flat_text = text.reshape(images * tokens, features)
    mid, out, wide_one, wide_two, stats = made
    cot, wide_grad, loss = attention(
        mp, lengths, noise, flat_text, kv_weight, far, mid, stats, w_query, w_output, w_head
    )
    counts = (
        2 * half * width,
        conv_one.shape[0] * conv_one.shape[1],
        images * lax.axis_size(DP_MP) * clean.shape[0] * clean.shape[2],
    )
    conv_one_update, conv_two_update, kv, mean = finish(
        counts, flat_text, cot, loss, out, wide_one, wide_two, wide_grad, stats, conv_two
    )
    return (conv_one_update, conv_two_update, kv.T, mean[0, 0])


def solution(mesh):
    finer = Mesh(
        mesh.devices.reshape(2, 4, 4, 2, mesh.shape["mp"]), ("dp_0", "dp_1", "dp_2", "dp_3", "mp")
    )
    placed = (
        P(DP_MP, None, None),
        P(DP_MP, None, None),
        P(DP_MP, None, None),
        P(DP_MP, None, None),
        P(DP_MP),
        P(DP_MP),
        P(DP_MP),
        P(DP_MP, None, None),
        P(),
        P(),
        P(),
        P(),
        P("mp", None),
        P(),
        P(),
        P(),
    )
    return jax.shard_map(
        local,
        mesh=finer,
        in_specs=placed,
        out_specs=(P(DP_MP, None), P(DP_MP, None), P("mp", DP), P()),
        check_vma=False,
    )
```

```python
import functools
import math

import jax
import jax.numpy as jnp
import numpy as np
from jax import lax
from jax.sharding import Mesh
from jax.sharding import PartitionSpec as P
from jax.experimental import pallas as pl
from jax.experimental.pallas import tpu as pltpu

S = 64
GROUPS = 32
HEADS = 2
HEAD_DIM = 64
FREQS = 64
STEPS = 1000
DP_MP = ("dp_0", "dp_1", "dp_2", "dp_3", "mp")
DP = ("dp_0", "dp_1", "dp_2", "dp_3")


PIXELS = S * S
CHUNK = 2048
CHUNKS = PIXELS // CHUNK
EDGE = S
C = 128


def group_total(line):
    lane = lax.broadcasted_iota(jnp.int32, line.shape, 1)
    pair = line + jnp.where(
        lane % 2 == 0, pltpu.roll(line, C - 1, 1), pltpu.roll(line, 1, 1)
    )
    return pair + jnp.where(
        lane % 4 < 2, pltpu.roll(pair, C - 2, 1), pltpu.roll(pair, 2, 1)
    )


def group_mean(total):
    line = jnp.broadcast_to(jnp.sum(total, axis=0, keepdims=True), (8, C)) / PIXELS
    return group_total(line)[0:1] / (C // GROUPS)


def row_of(value, i):
    row = value[0:1]
    for r in range(1, value.shape[0]):
        row = jnp.where(i == r, value[r : r + 1], row)
    return row


def fold(value):
    return jnp.sum(value.reshape(-1, 8, value.shape[-1]), axis=0)


def spread(act):
    column = lax.broadcasted_iota(jnp.int32, act.shape, 0) % S
    rows = act.shape[0]
    left = jnp.where(column == 0, 0.0, pltpu.roll(act, 1, 0))
    right = jnp.where(column == S - 1, 0.0, pltpu.roll(act, rows - 1, 0))
    return jnp.concatenate(
        [left.astype(jnp.bfloat16), act.astype(jnp.bfloat16), right.astype(jnp.bfloat16)], axis=1
    )


def span(j, size=CHUNK):
    return pl.ds(pl.multiple_of(j * size, size), size)


LINES = CHUNK // S


def inside(j, shift=1):
    return pl.ds(j * LINES + shift, LINES)


def clear_edges(ref, i):
    zero = jnp.zeros((S, ref.shape[-1]), jnp.bfloat16)
    ref[i, 0] = zero
    ref[i, S + 1] = zero


CONV = 2048
PAIRS = CONV // (2 * S)


def fill_pairs(pair_ref, block_of):
    for iy in range(4):
        for dx in range(3):
            at = (iy * 3 + dx) * C
            for oy in range(2):
                dy = iy - oy
                block = (
                    block_of(dy * 3 + dx) if 0 <= dy < 3 else jnp.zeros((C, C), jnp.bfloat16)
                )
                pair_ref[at : at + C, oy * C : (oy + 1) * C] = block


def conv_rows(wide_ref, i, j, pair_ref):
    rows = [
        jnp.concatenate([wide_ref[i, 2 * (j * PAIRS + t) + iy] for iy in range(4)], axis=1)
        for t in range(PAIRS)
    ]
    value = jnp.dot(
        jnp.concatenate(rows, axis=0), pair_ref[...], preferred_element_type=jnp.float32
    )
    lines = []
    for t in range(PAIRS):
        for oy in range(2):
            lines.append(value[t * S : (t + 1) * S, oy * C : (oy + 1) * C])
    return jnp.concatenate(lines, axis=0)


def loop_sum(body, size=CHUNK):
    return lax.fori_loop(0, PIXELS // size, body, jnp.zeros((8, C), jnp.float32))


def forward_kernel(
    feature_ref,
    clean_in,
    noise_in,
    low_in,
    aug_in,
    stem_in,
    time_in,
    one_in,
    two_in,
    mid_ref,
    out_ref,
    wide_one,
    wide_two,
    stats_ref,
    clean_ref,
    noise_ref,
    low_ref,
    aug_ref,
    stem_ref,
    time_ref,
    one_ref,
    two_ref,
    planes_ref,
    stems_ref,
    embed_ref,
    lhs_ref,
    pair_one,
    pair_two,
    sems,
):
    sources = (stem_in, time_in, clean_in, noise_in, low_in, aug_in, one_in, two_in)
    targets = (stem_ref, time_ref, clean_ref, noise_ref, low_ref, aug_ref, one_ref, two_ref)
    copies = [
        pltpu.make_async_copy(sources[n], targets[n], sems.at[n]) for n in range(len(sources))
    ]
    for copy in copies:
        copy.start()
    images = clean_ref.shape[1]
    for copy in copies:
        copy.wait()
    fill_pairs(pair_one, lambda tap: one_ref[tap * C : (tap + 1) * C])
    fill_pairs(pair_two, lambda tap: two_ref[tap * C : (tap + 1) * C])
    w = jnp.concatenate([stem_ref[...], jnp.zeros((2, C), jnp.float32)], axis=0)
    w1 = w.astype(jnp.bfloat16).astype(jnp.float32)
    w2 = (w - w1).astype(jnp.bfloat16).astype(jnp.float32)
    w3 = w - w1 - w2
    stems_ref[...] = jnp.concatenate([w1, w2, w1, w3, w2, w1], axis=0).astype(jnp.bfloat16)
    feature = jnp.concatenate(
        [feature_ref[:, : 2 * C], jnp.zeros((8 - images, 2 * C), jnp.float32)], axis=0
    )
    embed = jnp.dot(
        feature,
        time_ref[...],
        precision=lax.Precision.HIGHEST,
        preferred_element_type=jnp.float32,
    )
    embed_ref[...] = embed * jax.nn.sigmoid(embed)
    planes_ref[...] = jnp.zeros(planes_ref.shape, jnp.float32)

    def image(i, carry):
        coefs = [row_of(feature_ref[:, 2 * C + k : 2 * C + k + 1], i) for k in range(4)]
        for k in range(3):
            planes_ref[k : k + 1] = (
                coefs[0] * row_of(clean_ref[k], i)
                + coefs[1] * row_of(noise_ref[k], i)
            )
            planes_ref[3 + k : 4 + k] = (
                coefs[2] * row_of(low_ref[k], i) + coefs[3] * row_of(aug_ref[k], i)
            )
        s = planes_ref[...]
        s1 = s.astype(jnp.bfloat16).astype(jnp.float32)
        s2 = (s - s1).astype(jnp.bfloat16).astype(jnp.float32)
        s3 = s - s1 - s2
        lhs_ref[...] = jnp.concatenate([s1, s1, s2, s1, s2, s3], axis=0).astype(jnp.bfloat16)
        clear_edges(wide_one, i)
        clear_edges(wide_two, i)

        def stem(j, total):
            h = lax.dot_general(
                lhs_ref[:, span(j)],
                stems_ref[...],
                (((0,), (0,)), ((), ())),
                preferred_element_type=jnp.float32,
            )
            mid_ref[i, span(j)] = h
            return total + fold(h)

        def variance(ref, mean):
            def body(j, total):
                centred = ref[i, span(j)] - mean
                return total + fold(centred * centred)

            return lax.rsqrt(group_mean(loop_sum(body)) + 1e-05)

        mean_one = group_mean(loop_sum(stem))
        inv_one = variance(mid_ref, mean_one)

        def first(j, carry):
            act = (mid_ref[i, span(j)] - mean_one) * inv_one
            wide_one[i, inside(j)] = spread(act * jax.nn.sigmoid(act)).reshape(LINES, S, 3 * C)
            return carry

        lax.fori_loop(0, CHUNKS, first, 0)

        def conv_first(j, total):
            value = conv_rows(wide_one, i, j, pair_one)
            out_ref[i, span(j, CONV)] = value
            return total + fold(value)

        mean_two = group_mean(loop_sum(conv_first, CONV))
        inv_two = variance(out_ref, mean_two)
        gain = 1.0 + row_of(embed_ref[0:images, 0:C], i)
        shift = row_of(embed_ref[0:images, C : 2 * C], i)

        def next_act(j, carry):
            act = (out_ref[i, span(j)] - mean_two) * inv_two * gain + shift
            wide_two[i, inside(j)] = spread(act * jax.nn.sigmoid(act)).reshape(LINES, S, 3 * C)
            return carry

        lax.fori_loop(0, CHUNKS, next_act, 0)

        def conv_second(j, total):
            value = mid_ref[i, span(j, CONV)] + conv_rows(wide_two, i, j, pair_two)
            mid_ref[i, span(j, CONV)] = value
            return total + fold(value)

        mean_three = group_mean(loop_sum(conv_second, CONV))
        inv_three = variance(mid_ref, mean_three)
        stats_ref[i] = jnp.concatenate(
            [mean_two, inv_two, mean_three, inv_three, gain, shift, gain, shift], axis=0
        )
        return carry

    lax.fori_loop(0, images, image, 0)


def forward(feature, *arrays):
    images = feature.shape[0]
    bf16, f32 = jnp.bfloat16, jnp.float32
    wide = jax.ShapeDtypeStruct((images, S + 2, S, 3 * C), bf16)
    flat = jax.ShapeDtypeStruct((images, PIXELS, C), f32)
    return pl.pallas_call(
        forward_kernel,
        out_shape=(flat, flat, wide, wide, jax.ShapeDtypeStruct((images, 8, C), f32)),
        in_specs=[pl.BlockSpec(memory_space=pltpu.VMEM)]
        + [pl.BlockSpec(memory_space=pltpu.HBM)] * 8,
        out_specs=[pl.BlockSpec(memory_space=pltpu.VMEM)] * 5,
        scratch_shapes=[pltpu.VMEM(a.shape, a.dtype) for a in arrays]
        + [
            pltpu.VMEM((8, PIXELS), f32),
            pltpu.VMEM((48, C), bf16),
            pltpu.VMEM((8, 2 * C), f32),
            pltpu.VMEM((48, PIXELS), bf16),
            pltpu.VMEM((12 * C, 2 * C), bf16),
            pltpu.VMEM((12 * C, 2 * C), bf16),
            pltpu.SemaphoreType.DMA((8,)),
        ],
        compiler_params=pltpu.CompilerParams(vmem_limit_bytes=LIMIT_F * 2**20),
        cost_estimate=pl.CostEstimate(
            flops=10**10, bytes_accessed=22 * 10**6, transcendentals=2 * 10**6
        ),
        name="forward",
    )(feature, *(pltpu.with_memory_space_constraint(a, pltpu.HBM) for a in arrays))


TN = (((0,), (0,)), ((), ()))
NT = (((1,), (1,)), ((), ()))


def mm(a, b, dims=(((1,), (0,)), ((), ()))):
    return lax.dot_general(a, b, dims, preferred_element_type=jnp.float32)


def attend_kernel(
    half_ref,
    lengths_ref,
    noise_ref,
    text_ref,
    near_ref,
    far_ref,
    mid_ref,
    stats_ref,
    query_ref,
    output_ref,
    heads_ref,
    cot_ref,
    wide_grad,
    loss_ref,
    kv_ref,
    key_ref,
    val_ref,
    dkey_ref,
    dval_ref,
    dnorm_ref,
    dout_ref,
    head_ref,
    goal_ref,
):
    bf16, f32 = jnp.bfloat16, jnp.float32
    images = noise_ref.shape[1]
    tokens = text_ref.shape[0] // images
    half = near_ref.shape[0]
    mp = half_ref[0]
    here = pl.ds(pl.multiple_of(mp * half, half), half)
    there = pl.ds(pl.multiple_of((1 - mp) * half, half), half)
    kv_ref[...] = (
        mm(text_ref[:, here], near_ref[...]) + mm(text_ref[:, there], far_ref[...])
    ).astype(bf16)
    head_ref[...] = jnp.concatenate(
        [heads_ref[...].astype(f32), jnp.zeros((8 - heads_ref.shape[0], C), f32)], axis=0
    ).astype(bf16)
    goal_ref[...] = jnp.zeros(goal_ref.shape, f32)
    lane = lax.broadcasted_iota(jnp.int32, (tokens, C), 1)
    nothing = jnp.zeros((8, C), f32)

    def image(i, loss):
        clear_edges(wide_grad, i)
        for k in range(3):
            goal_ref[k : k + 1] = row_of(noise_ref[k], i)
        both = kv_ref[pl.ds(pl.multiple_of(i * tokens, tokens), tokens), :]
        zero = jnp.zeros((tokens, C), bf16)
        low = lane < HEAD_DIM
        key_ref[...] = jnp.concatenate(
            [jnp.where(low, both[:, :C], zero), jnp.where(low, zero, both[:, :C])], axis=0
        )
        val_ref[...] = jnp.concatenate(
            [jnp.where(low, both[:, C:], zero), jnp.where(low, zero, both[:, C:])], axis=0
        )
        dkey_ref[...] = jnp.zeros(dkey_ref.shape, f32)
        dval_ref[...] = jnp.zeros(dval_ref.shape, f32)
        mean_three, inv_three = stats_ref[i, 2:3], stats_ref[i, 3:4]
        keep = lax.broadcasted_iota(jnp.int32, (ATTEND, tokens), 1) < lengths_ref[i]

        def attend(j, carry):
            total, moment, loss = carry
            mid = mid_ref[i, span(j, ATTEND)]
            hat = (mid - mean_three) * inv_three
            query = (mm(hat.astype(bf16), query_ref[...]) * HEAD_DIM ** (-0.5)).astype(bf16)
            scores = mm(query, key_ref[...], NT)
            probs = []
            for h in range(HEADS):
                one = jnp.where(keep, scores[:, h * tokens : (h + 1) * tokens], -1e30)
                one = jnp.exp(one - jnp.max(one, axis=1, keepdims=True))
                probs.append(one / jnp.sum(one, axis=1, keepdims=True))
            rounded = jnp.concatenate([p.astype(bf16) for p in probs], axis=1)
            attended = mm(rounded, val_ref[...]).astype(bf16)
            out = (mid + mm(attended, output_ref[...])).astype(bf16)
            pred = mm(out, head_ref[...], NT)
            error = pred - goal_ref[:, span(j, ATTEND)].T
            loss = loss + fold(error * error)
            dout = mm((2.0 * error).astype(bf16), head_ref[...]).astype(bf16)
            dout_ref[span(j, ATTEND)] = dout
            datt = mm(dout, output_ref[...], NT).astype(bf16)
            dprobs = mm(datt, val_ref[...], NT).astype(bf16).astype(f32)
            dval_ref[...] += mm(datt, rounded, TN)
            dscores = []
            for h in range(HEADS):
                one = dprobs[:, h * tokens : (h + 1) * tokens]
                inner = jnp.sum(one * probs[h], axis=1, keepdims=True)
                dscores.append((probs[h] * (one - inner)).astype(bf16))
            dscores = jnp.concatenate(dscores, axis=1)
            dkey_ref[...] += mm(query, dscores, TN)
            dquery = mm(dscores, key_ref[...]).astype(bf16)
            dnorm = (mm(dquery, query_ref[...], NT) * HEAD_DIM ** (-0.5)).astype(bf16)
            dnorm_ref[span(j, ATTEND)] = dnorm
            dnorm = dnorm.astype(f32)
            return (total + fold(dnorm), moment + fold(dnorm * hat), loss)

        total, moment, loss = lax.fori_loop(0, PIXELS // ATTEND, attend, (nothing, nothing, loss))
        low_row = lax.broadcasted_iota(jnp.int32, (C, tokens), 0) < HEAD_DIM
        cots = [
            jnp.where(low_row, ref[:, :tokens], ref[:, tokens:]) for ref in (dkey_ref, dval_ref)
        ]
        cot_ref[:, pl.ds(pl.multiple_of(i * tokens, tokens), tokens)] = jnp.concatenate(
            cots, axis=0
        ).astype(bf16)
        first, second = group_mean(total), group_mean(moment)

        def middle(j, carry):
            hat = (mid_ref[i, span(j)] - mean_three) * inv_three
            grad = dout_ref[span(j)].astype(f32) + inv_three * (
                dnorm_ref[span(j)].astype(f32) - first - hat * second
            )
            wide_grad[i, inside(j)] = spread(grad).reshape(LINES, S, 3 * C)
            return carry

        lax.fori_loop(0, CHUNKS, middle, 0)

        return loss

    loss = lax.fori_loop(0, images, image, jnp.zeros((8, 8), f32))
    loss_ref[...] = jnp.broadcast_to(
        jnp.sum(jnp.sum(loss, axis=0, keepdims=True), axis=1, keepdims=True) / C, (1, C)
    )


def attention(half, lengths, noise, text, near, far, mid, stats, w_query, w_output, head):
    images = noise.shape[1]
    bf16, f32 = jnp.bfloat16, jnp.float32
    tokens = text.shape[0] // images
    vmem = pl.BlockSpec(memory_space=pltpu.VMEM)
    smem = pl.BlockSpec(memory_space=pltpu.SMEM)
    return pl.pallas_call(
        attend_kernel,
        out_shape=(
            jax.ShapeDtypeStruct((2 * C, images * tokens), bf16),
            jax.ShapeDtypeStruct((images, S + 2, S, 3 * C), bf16),
            jax.ShapeDtypeStruct((1, C), f32),
        ),
        in_specs=[smem] * 2 + [vmem] * 9,
        out_specs=[vmem] * 3,
        scratch_shapes=[
            pltpu.VMEM((images * tokens, 2 * C), bf16),
            pltpu.VMEM((2 * tokens, C), bf16),
            pltpu.VMEM((2 * tokens, C), bf16),
            pltpu.VMEM((C, 2 * tokens), f32),
            pltpu.VMEM((C, 2 * tokens), f32),
            pltpu.VMEM((PIXELS, C), bf16),
            pltpu.VMEM((PIXELS, C), bf16),
            pltpu.VMEM((8, C), bf16),
            pltpu.VMEM((8, PIXELS), f32),
        ],
        compiler_params=pltpu.CompilerParams(vmem_limit_bytes=LIMIT_A * 2**20),
        cost_estimate=pl.CostEstimate(
            flops=10**10, bytes_accessed=16 * 10**6, transcendentals=6 * 10**6
        ),
        name="attention",
    )(half, lengths, noise, text, near, far, mid, stats, w_query, w_output, head)


ATTEND = 4096
LIMIT_F = 12
LIMIT_A = 20
LIMIT_T = 20


MESH = pl.DeviceIdType.MESH
LINE = 4
WIDTHS = (256, 256, 128, 128)
ORDERS = (("x", "y", "z"), ("y", "z", "x"), ("z", "x", "y"), ("z", "x", "y"))
COLUMNS = (0, 256, 640, 512)


def axis_target(axis, to):
    if axis == "x":
        return {"dp_1": to}
    if axis == "y":
        return {"dp_2": to}
    if axis == "z":
        return {"dp_0": to // 2, "mp": lax.rem(to, 2)}
    return {"dp_3": to}


def remote(source, target, send, recv, axis, to):
    copy = pltpu.make_async_remote_copy(
        src_ref=source,
        dst_ref=target,
        send_sem=send,
        recv_sem=recv,
        device_id=axis_target(axis, to),
        device_id_type=MESH,
    )
    copy.start()
    return copy


def finish_kernel(
    counts,
    text_ref,
    cot_ref,
    loss_ref,
    out_ref,
    wide_one,
    wide_two,
    wide_grad,
    stats_ref,
    two_ref,
    one_out,
    two_out,
    kv_out,
    mean_out,
    rows_ref,
    dhat_ref,
    grad_ref,
    flat_ref,
    sum_ref,
    flip_ref,
    grad_pad,
    total_ref,
    slots,
    send_sems,
    recv_sems,
    slot_send,
    slot_recv,
    *stages,
):
    bf16, f32 = jnp.bfloat16, jnp.float32
    images = stats_ref.shape[0]
    own, core_in, held, line_in, second, second_in, third, third_in = (
        stages[n * 4 : (n + 1) * 4] for n in range(8)
    )
    place = {
        "x": lax.axis_index("dp_1"),
        "y": lax.axis_index("dp_2"),
        "z": lax.axis_index("dp_0") * 2 + lax.axis_index("mp"),
        "core": lax.axis_index("dp_3"),
    }
    core = place["core"]
    other = 1 - core
    barrier = pltpu.get_barrier_semaphore()
    for outer, inner, size in (("z", "core", 2), ("x", "y", LINE)):
        for k in range(1, LINE * size):
            to = {
                **axis_target(outer, lax.rem(place[outer] + k // size, LINE)),
                **axis_target(inner, lax.rem(place[inner] + k % size, size)),
            }
            pl.semaphore_signal(barrier, inc=1, device_id=to, device_id_type=MESH)

    sent = []

    def start_core(c):
        copy = remote(
            own[c].at[other],
            core_in[c],
            send_sems.at[c * 10],
            recv_sems.at[c * 10],
            "core",
            other,
        )
        sent.append(copy)
        return [copy]

    def part_of(left, axis, at):
        return tuple(at if name == axis else slice(None) for name in left)

    def exchange(c, stage, source, left, into):
        axis = ORDERS[c][stage]
        started = []
        for k in range(1, LINE):
            to = lax.rem(place[axis] + k, LINE)
            slot = c * 10 + stage * 3 + k
            started.append(
                remote(
                    source[c].at[part_of(left, axis, to)],
                    into[c].at[k - 1],
                    send_sems.at[slot],
                    recv_sems.at[slot],
                    axis,
                    to,
                )
            )
        sent.extend(started)
        return started

    def arrive(copies):
        for copy in copies:
            copy.wait_recv()

    def to_first(c, copies):
        arrive(copies)

        def add(i, carry):
            held[c][i] = (own[c][core, i].astype(f32) + core_in[c][i].astype(f32)).astype(bf16)
            return carry

        lax.fori_loop(0, LINE, add, 0)
        return exchange(c, 0, held, ("x", "y", "z"), line_in)

    def to_second(c, copies):
        arrive(copies)
        axis = ORDERS[c][0]
        rest = [name for name in ("x", "y", "z") if name != axis]
        for i in range(LINE):
            index = tuple(
                place[axis] if name == axis else (i if name == rest[0] else slice(None))
                for name in ("x", "y", "z")
            )
            value = held[c][index].astype(f32)
            for k in range(LINE - 1):
                value = value + line_in[c][k, i].astype(f32)
            second[c][i] = value.astype(bf16)
        return exchange(c, 1, second, tuple(rest), second_in)

    def to_third(c, copies):
        arrive(copies)
        left = tuple(name for name in ("x", "y", "z") if name != ORDERS[c][0])
        axis = ORDERS[c][1]
        value = second[c][part_of(left, axis, place[axis])].astype(f32)
        for k in range(LINE - 1):
            value = value + second_in[c][k].astype(f32)
        third[c][...] = value.astype(bf16)
        return exchange(c, 2, third, (ORDERS[c][2],), third_in)

    def to_total(c, copies):
        arrive(copies)
        value = third[c][place[ORDERS[c][2]]].astype(f32)
        for k in range(LINE - 1):
            value = value + third_in[c][k].astype(f32)
        total_ref[:, COLUMNS[c] : COLUMNS[c] + WIDTHS[c]] = value

    tokens = cot_ref.shape[1]
    row = lax.broadcasted_iota(jnp.int32, (1024, 256), 0)
    col = lax.broadcasted_iota(jnp.int32, (1024, 256), 1)
    owner = ((row // 16) % 2 * 32 + row // 32 % 16 * 2 + row // 512) * 4 + row % 4
    pick = jnp.where(owner == col, 1.0, 0.0).astype(bf16)
    picked = mm(pick, cot_ref[...])
    quarter = (row // 4) % 4
    for q in range(4):
        rows_ref[:, q * tokens : (q + 1) * tokens] = jnp.where(
            quarter[:, :tokens] == q, picked, 0.0
        ).astype(bf16)

    def block(m, carry):
        for c in range(2):
            at = m * 2048 + c * 256
            wide = jnp.concatenate(
                [
                    text_ref[:, pl.ds(pl.multiple_of(at + q * 512, 256), 256)]
                    for q in range(4)
                ],
                axis=0,
            )
            for half in range(2):
                value = mm(rows_ref[half * 512 : (half + 1) * 512, :], wide).astype(bf16)
                value = value.reshape(4, 4, 2, 16, 256)
                for zh in range(2):
                    own[c][half, :, :, zh * 2 + m] = value[:, :, zh]
        return carry

    lax.fori_loop(0, 2, block, 0)
    pl.semaphore_wait(barrier, 22)
    first_kv = [start_core(0), start_core(1)]

    fill_pairs(flip_ref, lambda tap: two_ref[(8 - tap) * C : (9 - tap) * C].T)
    clear_edges(grad_pad, 0)
    sum_ref[...] = jnp.zeros(sum_ref.shape, f32)
    flat_ref[:, 9 * C :] = jnp.zeros((2, 16, C), f32)
    nothing = jnp.zeros((8, C), f32)

    def weights(which, i, source, grad_of):
        grad_ref[...] = jnp.zeros(grad_ref.shape, f32)

        def body(j, carry):
            grads = [grad_of(inside(j, 2 - dy)).reshape(CHUNK, C) for dy in range(3)]
            grad_ref[...] += mm(
                jnp.concatenate(grads, axis=1), source[i, inside(j)].reshape(CHUNK, 3 * C), TN
            )
            return carry

        lax.fori_loop(0, CHUNKS, body, 0)
        sum_ref[which] += grad_ref[...].astype(bf16).astype(f32)

    def pack(which, c):
        for dy in range(3):
            for dx in range(3):
                at = (dy * 3 + dx) * C
                flat_ref[which, at : at + C] = sum_ref[
                    which, dy * C : (dy + 1) * C, dx * C : (dx + 1) * C
                ].T
        row = lax.broadcasted_iota(jnp.int32, (16, C), 0)

        for d in range(128):
            piece = jnp.where(row < 9, flat_ref[which, d * 9 : d * 9 + 16], 0.0).astype(bf16)
            own[c][d // 2 % 2, d // 16 % 4, d // 4 % 4, d // 64 * 2 + d % 2] = piece

    def act_grad(i):
        mean_two, inv_two = stats_ref[i, 0:1], stats_ref[i, 1:2]
        gain, shift = stats_ref[i, 4:5], stats_ref[i, 5:6]

        def inner(j, carry):
            total, moment = carry
            dact = conv_rows(wide_grad, i, j, flip_ref).astype(bf16).astype(f32)
            at = span(j, CONV)
            hat = (out_ref[i, at] - mean_two) * inv_two
            act = hat * gain + shift
            gate = jax.nn.sigmoid(act)
            dhat = dact * (gate * (1.0 + act * (1.0 - gate))) * gain
            dhat_ref[at] = dhat
            return (total + fold(dhat), moment + fold(dhat * hat))

        total, moment = lax.fori_loop(0, PIXELS // CONV, inner, (nothing, nothing))
        return mean_two, inv_two, group_mean(total), group_mean(moment)

    def early_grad(i, lines):
        mean_two, inv_two, first, moment = lines

        def early(j, carry):
            hat = (out_ref[i, span(j)] - mean_two) * inv_two
            grad = inv_two * (dhat_ref[span(j)] - first - hat * moment)
            grad_pad[0, inside(j)] = grad.astype(bf16).reshape(LINES, S, C)
            return carry

        lax.fori_loop(0, CHUNKS, early, 0)
        weights(0, i, wide_one, lambda at: grad_pad[0, at])

    weights(1, 0, wide_two, lambda at: wide_grad[0, at, :, C : 2 * C])
    copies = [to_first(0, first_kv[0]), to_first(1, first_kv[1])]
    for i in range(1, images):
        weights(1, i, wide_two, lambda at, i=i: wide_grad[i, at, :, C : 2 * C])
    pack(1, 2)
    copies.append(start_core(2))
    lines = act_grad(0)
    copies[2] = to_first(2, copies[2])
    early_grad(0, lines)
    for c in range(2):
        copies[c] = to_second(c, copies[c])
    lines = act_grad(1)
    copies[2] = to_second(2, copies[2])
    for c in range(2):
        copies[c] = to_third(c, copies[c])
    early_grad(1, lines)
    pack(0, 3)
    copies.append(start_core(3))
    copies[2] = to_third(2, copies[2])
    for c in range(2):
        to_total(c, copies[c])
    copies[3] = to_first(3, copies[3])
    to_total(2, copies[2])
    copies[3] = to_second(3, copies[3])
    copies[3] = to_third(3, copies[3])
    to_total(3, copies[3])

    value = total_ref[...]
    square = value * value
    kv_line = jnp.sum(square[:, :512], axis=0, keepdims=True)
    kv_line = (
        kv_line[:, :128] + kv_line[:, 128:256] + kv_line[:, 256:384] + kv_line[:, 384:512]
    )
    conv_line = jnp.sum(square[:, 512:], axis=0, keepdims=True)
    row = lax.broadcasted_iota(jnp.int32, (8, 128), 0)
    tile = jnp.where(row == 0, kv_line, 0.0)
    tile = jnp.where(row == 1, conv_line[:, :128], tile)
    tile = jnp.where(row == 2, conv_line[:, 128:], tile)
    tile = jnp.where(row == 3, loss_ref[...], tile)
    at = 0
    for stage, (outer, inner) in enumerate((("z", "core"), ("x", "y"))):
        sizes = (LINE, 2 if inner == "core" else LINE)
        mine = place[outer] * sizes[1] + place[inner]
        slots[stage, mine] = tile
        started = []
        for k in range(1, sizes[0] * sizes[1]):
            to = {
                **axis_target(outer, lax.rem(place[outer] + k // sizes[1], LINE)),
                **axis_target(inner, lax.rem(place[inner] + k % sizes[1], sizes[1])),
            }
            copy = pltpu.make_async_remote_copy(
                src_ref=slots.at[stage, mine],
                dst_ref=slots.at[stage, mine],
                send_sem=slot_send.at[at],
                recv_sem=slot_recv.at[at],
                device_id=to,
                device_id_type=MESH,
            )
            copy.start()
            started.append(copy)
            at += 1
        arrive(started)
        sent.extend(started)
        tile = slots[stage, 0]
        for k in range(1, sizes[0] * sizes[1]):
            tile = tile + slots[stage, k]
    sums = jnp.sum(tile, axis=1, keepdims=True)
    kv_scale = lax.rsqrt(sums[0:1] / counts[0] + 1e-06)
    one_scale = lax.rsqrt(sums[1:2] / counts[1] + 1e-06)
    two_scale = lax.rsqrt(sums[2:3] / counts[1] + 1e-06)
    one_out[...] = total_ref[0:9, 512:640] * one_scale
    two_out[...] = total_ref[0:9, 640:768] * two_scale
    for q in range(4):
        kv_out[:, q * 512 : (q + 1) * 512] = total_ref[q * 4 : (q + 1) * 4, 0:512] * kv_scale
    mean_out[...] = jnp.broadcast_to(sums[3:4] / counts[2], mean_out.shape)
    for copy in sent:
        copy.wait_send()


def finish(counts, *arrays):
    bf16, f32 = jnp.bfloat16, jnp.float32
    vmem = pl.BlockSpec(memory_space=pltpu.VMEM)
    stages = [
        (2, 4, 4, 4, 16),
        (4, 4, 4, 16),
        (4, 4, 4, 16),
        (3, 4, 4, 16),
        (4, 4, 16),
        (3, 4, 16),
        (4, 16),
        (3, 16),
    ]
    return pl.pallas_call(
        functools.partial(finish_kernel, counts),
        out_shape=(
            jax.ShapeDtypeStruct((9, 128), f32),
            jax.ShapeDtypeStruct((9, 128), f32),
            jax.ShapeDtypeStruct((4, 2048), f32),
            jax.ShapeDtypeStruct((1, 128), f32),
        ),
        in_specs=[vmem] * len(arrays),
        out_specs=[vmem] * 4,
        scratch_shapes=[
            pltpu.VMEM((1024, 1024), bf16),
            pltpu.VMEM((PIXELS, C), f32),
            pltpu.VMEM((3 * C, 3 * C), f32),
            pltpu.VMEM((2, 9 * C + 16, C), f32),
            pltpu.VMEM((2, 3 * C, 3 * C), f32),
            pltpu.VMEM((12 * C, 2 * C), bf16),
            pltpu.VMEM((1, S + 2, S, C), bf16),
            pltpu.VMEM((16, 768), f32),
            pltpu.VMEM((2, 16, 8, 128), f32),
            pltpu.SemaphoreType.DMA((40,)),
            pltpu.SemaphoreType.DMA((40,)),
            pltpu.SemaphoreType.DMA((22,)),
            pltpu.SemaphoreType.DMA((22,)),
        ]
        + [pltpu.VMEM((*shape, width), bf16) for shape in stages for width in WIDTHS],
        compiler_params=pltpu.CompilerParams(
            collective_id=0, has_side_effects=True, vmem_limit_bytes=LIMIT_T * 2**20
        ),
        cost_estimate=pl.CostEstimate(
            flops=2 * 10**10, bytes_accessed=30 * 10**6, transcendentals=2 * 10**6
        ),
        name="finish",
    )(*arrays)


def local(
    clean,
    noise,
    lowres,
    aug_noise,
    timesteps,
    aug_levels,
    lengths,
    text,
    w_stem,
    w_time,
    conv_one,
    conv_two,
    kv_weight,
    w_query,
    w_output,
    w_head,
):
    images = clean.shape[0]
    tokens = text.shape[1]
    features = text.shape[2]
    width = kv_weight.shape[1]
    half = kv_weight.shape[0]
    bf16, f32 = jnp.bfloat16, jnp.float32
    far = lax.ppermute(kv_weight, "mp", [(0, 1), (1, 0)])

    step, level = timesteps[:, None], aug_levels[:, None]
    width_f = 4 * FREQS
    lane = np.arange(width_f + C)
    coef = lane >= width_f
    on_step = np.where(coef, (lane - width_f) < 2, lane < 2 * FREQS)
    index = jnp.where(on_step, step, level).astype(f32)
    freqs = jnp.exp(-math.log(10000.0) * (lane % FREQS).astype(np.float32) / FREQS)
    ratio = (index / STEPS + 0.008) / 1.008
    angles = jnp.where(coef, ratio * (math.pi / 2.0), index * freqs)
    cosine = jnp.cos(angles)
    signal = cosine * cosine
    signal = jnp.sqrt(jnp.where(lane % 2 == 0, signal, 1.0 - signal))
    wave = jnp.where(lane % (2 * FREQS) < FREQS, jnp.sin(angles), cosine)
    feature = jnp.where(coef, signal, wave)
    clean, noise, lowres, aug_noise = (
        jnp.transpose(a, (1, 0, 2)) for a in (clean, noise, lowres, aug_noise)
    )
    made = forward(
        feature, clean, noise, lowres, aug_noise, w_stem, w_time, conv_one, conv_two
    )
    mp = lax.axis_index("mp").astype(jnp.int32).reshape(1)
    flat_text = text.reshape(images * tokens, features)
    mid, out, wide_one, wide_two, stats = made
    cot, wide_grad, loss = attention(
        mp, lengths, noise, flat_text, kv_weight, far, mid, stats, w_query, w_output, w_head
    )
    counts = (
        2 * half * width,
        conv_one.shape[0] * conv_one.shape[1],
        images * lax.axis_size(DP_MP) * clean.shape[0] * clean.shape[2],
    )
    conv_one_update, conv_two_update, kv, mean = finish(
        counts, flat_text, cot, loss, out, wide_one, wide_two, wide_grad, stats, conv_two
    )
    return (conv_one_update, conv_two_update, kv.T, mean[0, 0])


def solution(mesh):
    finer = Mesh(
        mesh.devices.reshape(2, 4, 4, 2, mesh.shape["mp"]), ("dp_0", "dp_1", "dp_2", "dp_3", "mp")
    )
    placed = (
        P(DP_MP, None, None),
        P(DP_MP, None, None),
        P(DP_MP, None, None),
        P(DP_MP, None, None),
        P(DP_MP),
        P(DP_MP),
        P(DP_MP),
        P(DP_MP, None, None),
        P(),
        P(),
        P(),
        P(),
        P("mp", None),
        P(),
        P(),
        P(),
    )
    return jax.shard_map(
        local,
        mesh=finer,
        in_specs=placed,
        out_specs=(P(DP_MP, None), P(DP_MP, None), P("mp", DP), P()),
        check_vma=False,
    )
```
